128 devices in a mesh: dp: 8 (over y, core), expert: 16 (over z, x).
Axes of the slice: x: 4, y: 4, z: 4, core: 2. Of those that a mesh axis runs over, the one named last changes fastest.
Arguments:
- tokens: bfloat16 [8, 4, 8192, 1024], P('dp', None, 'expert'), may hold values from -8000 to 8000
- slot_params: bfloat16 [1024, 256], replicated, may hold values from -8 to 8
- dest: int32 [8, 4, 32], P('dp', None, 'expert'), may hold values from 0 to 127, as said below
- lengths: int32 [8, 4], P('dp'), may hold values from 256 to 8192
- w_in: bfloat16 [128, 1024, 4096], P('expert', None, 'dp'), may hold values from -0.1875 to 0.1875
- w_out: bfloat16 [128, 4096, 1024], P('expert', 'dp'), may hold values from -3 to 3
Outputs:
- mixed: bfloat16 [8, 128, 256, 1024], P('dp', 'expert')
The draws below stay inside these ranges and needn't reach their ends.
Inputs may be any that keep to these rules, and one draw needn't show every extreme that they name: For each g, dest[g] holds every number of 0 to 127 once; the 8 blocks held by one device (block indices j from k * 2 on, for every q) go to output blocks of different devices, device d holding output blocks d * 4 * 2 onward, so each device receives at most one block from each device.
All inputs are finite; a program needn't handle non-finite values.
Results may differ from the reference program's by a relative error of at most 0.01.
Values may be sent and summed in bfloat16 or wider, within the bound.
No kernel may reach another device: no remote copies, remote signals or barrier semaphores. Data moves between devices by JAX's collectives and lax.ppermute only.
A program may use at most 128 MiB of HBM per device.

```python
import math
import jax
import jax.numpy as jnp
from jax import lax

D = 1024
H = 4096
SLOTS = 2
BT = 256
SEQ_DP = 4
BLK_DEV = 2
EXPERTS = 128
GROUPS = 8
SHARDS = 16
LEN = 8192


def shared_columns(key):
    base = jax.random.normal(jax.random.fold_in(key, 11), (D, EXPERTS * SLOTS), jnp.float32) * (0.3 / math.sqrt(D))
    return base


def draw_slot_params(key, part):
    return shared_columns(key).astype(jnp.bfloat16)


def draw_tokens(key, part):
    slot_count = EXPERTS * SLOTS
    noise = jnp.clip(jax.random.normal(jax.random.fold_in(key, 21), (GROUPS, SEQ_DP, LEN, D), jnp.float32), -6.0, 6.0)
    peaked = jax.random.bernoulli(jax.random.fold_in(key, 24), 0.5, (GROUPS, SEQ_DP, LEN, 1))
    spread = jnp.where(peaked, 2.5, 5.0)
    columns = shared_columns(key).T
    norms = jnp.sum(columns * columns, axis=1)
    unit_columns = columns / norms[:, None]
    chosen = jax.random.randint(jax.random.fold_in(key, 25), (GROUPS, SEQ_DP, LEN), 0, slot_count)
    boost = 7.0 * jnp.take(unit_columns, chosen, axis=0)
    base = noise * spread + jnp.where(peaked, boost, 0.0)
    return base.astype(jnp.bfloat16)


def draw_w_out(key, part):
    common = jnp.clip(jax.random.normal(jax.random.fold_in(key, 41), (H, D), jnp.float32), -5.0, 5.0) * (4.0 / math.sqrt(H))
    own = jnp.clip(jax.random.normal(jax.random.fold_in(key, 42), (EXPERTS, H, D), jnp.float32), -5.0, 5.0) * (1.0 / math.sqrt(H))
    return (common[None, :, :] + own).astype(jnp.bfloat16)


def draw_dest(key, part):
    per_device = SEQ_DP * BLK_DEV
    group_keys = jax.random.split(jax.random.fold_in(key, 31), GROUPS)
    shifts = jax.vmap(lambda k: jax.random.permutation(k, SHARDS)[:per_device])(group_keys).astype(jnp.int32)
    source_keys = jax.random.split(jax.random.fold_in(key, 32), GROUPS * SHARDS)
    source_order = jax.vmap(lambda k: jax.random.permutation(k, per_device))(source_keys).reshape(GROUPS, SHARDS, per_device).astype(jnp.int32)
    target_keys = jax.random.split(jax.random.fold_in(key, 33), GROUPS * SHARDS)
    target_order = jax.vmap(lambda k: jax.random.permutation(k, per_device))(target_keys).reshape(GROUPS, SHARDS, per_device).astype(jnp.int32)
    sources = jnp.arange(SHARDS, dtype=jnp.int32)
    receiver = (sources[None, :, None] + shifts[:, None, :]) % SHARDS
    group_index = jnp.arange(GROUPS, dtype=jnp.int32)[:, None, None]
    within = target_order[group_index, receiver, jnp.arange(per_device, dtype=jnp.int32)[None, None, :]]
    values = receiver * per_device + within
    table = jnp.zeros((GROUPS, SHARDS, per_device), jnp.int32)
    table = table.at[group_index, sources[None, :, None], source_order].set(values)
    table = table.reshape(GROUPS, SHARDS, SEQ_DP, BLK_DEV).transpose(0, 2, 1, 3)
    return table.reshape(GROUPS, SEQ_DP, SHARDS * BLK_DEV).astype(jnp.int32)


def place_ends(entries, stream_key, least, top_value):
    dims = entries.shape
    place = [jax.random.randint(jax.random.fold_in(stream_key, axis), (), 0, dims[axis]) for axis in range(len(dims))]
    entries = entries.at[tuple(place)].set(least)
    longest = dims.index(max(dims))
    place[longest] = (place[longest] + 1) % dims[longest]
    return entries.at[tuple(place)].set(top_value)


def block_levels(rng, shape, cuts, smallest, high):
    def one(axis_at, blocks):
        steps = jax.random.uniform(jax.random.fold_in(jax.random.fold_in(rng, 6), axis_at), (blocks,), jnp.float32, smallest / len(cuts), high / len(cuts))
        return jnp.repeat(jnp.exp(steps), shape[axis_at] // blocks).reshape((-1,) + (1,) * (len(shape) - axis_at - 1))

    loudness = one(*cuts[0])
    for cut in cuts[1:]:
        loudness = loudness * one(*cut)
    return loudness


def normal_values(key, shape, scale, limit, cuts=(), kind=jnp.bfloat16):
    values = scale * jax.random.normal(key, shape, jnp.float32)
    if cuts:
        values = values * block_levels(key, shape, cuts, -0.22, 0.18)
    return jnp.clip(values, -limit, limit).astype(kind)


def setup_inputs(seed: int = 0) -> dict:
    key_list = jax.random.split(jax.random.key(seed), 7)
    tokens = draw_tokens(jax.random.fold_in(key_list[6], 71), 0)
    slot_params = draw_slot_params(jax.random.fold_in(key_list[6], 71), 0)
    dest = draw_dest(jax.random.fold_in(key_list[6], 71), 0)
    lengths = place_ends(jax.random.randint(key_list[3], (GROUPS, SEQ_DP), BT, LEN + 1), jax.random.fold_in(key_list[3], 1), BT, LEN).astype(jnp.int32)
    w_in = normal_values(key_list[4], (EXPERTS, D, H), D ** -0.5, 0.1875, ((0, 16), (2, 8)))
    w_out = draw_w_out(jax.random.fold_in(key_list[6], 71), 0)
    return {"tokens": tokens, "slot_params": slot_params, "dest": dest, "lengths": lengths, "w_in": w_in, "w_out": w_out}


def reference(tokens, slot_params, dest, lengths, w_in, w_out):
    groups, seqs, length, width = tokens.shape
    slots_total = slot_params.shape[1]
    experts = w_in.shape[0]
    per_expert = slots_total // experts
    block_count = length // BT
    position = jnp.arange(length, dtype=jnp.int32)
    flat_tokens = tokens.reshape(groups * seqs, length, width)
    flat_lengths = lengths.reshape(groups * seqs).astype(jnp.int32)

    def dispatch(args):
        feats, count = args
        live_mask = position < count
        logits = jnp.dot(feats, slot_params, preferred_element_type=jnp.float32)
        masked = jnp.where(live_mask[:, None], logits, -jnp.inf)
        top = jnp.max(masked, axis=0)
        weight = jnp.where(live_mask[:, None], jnp.exp(logits - top[None, :]), 0.0)
        mass = jnp.sum(weight, axis=0)
        numer = jnp.dot(weight.astype(jnp.bfloat16).T, feats, preferred_element_type=jnp.float32)
        return (numer / mass[:, None]).astype(jnp.bfloat16)

    slot_in = lax.map(dispatch, (flat_tokens, flat_lengths))
    by_expert = slot_in.reshape(groups * seqs, experts, per_expert, width)
    by_expert = by_expert.transpose(1, 0, 2, 3).reshape(experts, groups * seqs * per_expert, width)

    def expert_apply(args):
        rows_in, first, second = args
        hidden = jax.nn.gelu(jnp.dot(rows_in, first, preferred_element_type=jnp.float32)).astype(jnp.bfloat16)
        return jnp.dot(hidden, second, preferred_element_type=jnp.float32).astype(jnp.bfloat16)

    expert_rows = lax.map(expert_apply, (by_expert, w_in, w_out))
    slot_out = expert_rows.reshape(experts, groups * seqs, per_expert, width)
    slot_out = slot_out.transpose(1, 0, 2, 3).reshape(groups * seqs, slots_total, width)

    def combine(args):
        feats, count, outputs = args
        live_mask = position < count
        logits = jnp.dot(feats, slot_params, preferred_element_type=jnp.float32)
        mix = jax.nn.softmax(logits, axis=1).astype(jnp.bfloat16)
        result = jnp.dot(mix, outputs, preferred_element_type=jnp.float32)
        return jnp.where(live_mask[:, None], result, 0.0).astype(jnp.bfloat16)

    combined = lax.map(combine, (flat_tokens, flat_lengths, slot_out))
    blocks = combined.reshape(groups, seqs * block_count, BT, width)
    order = dest.reshape(groups, seqs * block_count).astype(jnp.int32)
    group_index = jnp.arange(groups, dtype=jnp.int32)[:, None]
    mixed = jnp.zeros_like(blocks).at[group_index, order].set(blocks)
    return mixed
```

```python
import functools
import math

import jax
import jax.numpy as jnp
from jax import lax
from jax.experimental import pallas as pl
from jax.experimental.pallas import tpu as pltpu
from jax.sharding import Mesh
from jax.sharding import PartitionSpec as P

DP = ("y", "c")
EXPERT = ("z", "x")
LANES = 128
PIECES = 8
NO_TOKEN = -1e30
F32 = jnp.float32
BF16 = jnp.bfloat16


def pieces_of(value):
    high = value.astype(BF16).astype(F32)
    rest = value - high
    middle = rest.astype(BF16).astype(F32)
    return high, middle, rest - middle


def dispatch_kernel(counts, peers, labels, tokens, params, payload, mixes, stats):
    q = pl.program_id(0)
    last = pl.num_programs(0) - 1
    feats = tokens[0, 0]
    length = feats.shape[0]
    shards = payload.shape[0]
    slots = params.shape[1]
    owned = slots // shards
    slabs = feats.shape[1] // LANES
    stat_rows = payload.shape[1] - owned
    seqs = stat_rows // (slabs * owned)
    block = mixes.shape[1]

    @pl.when(q == 0)
    def _():
        mixes[...] = jnp.zeros(mixes.shape, mixes.dtype)
        stats[...] = jnp.zeros(stats.shape, stats.dtype)

    logits = jnp.dot(feats, params[...], preferred_element_type=F32)
    live = lax.broadcasted_iota(jnp.int32, (length, 1), 0) < counts[q]
    masked = jnp.where(live, logits, NO_TOKEN)
    top = jnp.max(masked, axis=0, keepdims=True)
    weight = jnp.where(live, jnp.exp(masked - top), 0.0)
    mass = jnp.sum(weight, axis=0, keepdims=True)
    numer = lax.dot_general(
        weight.astype(BF16), feats, (((0,), (0,)), ((), ())), preferred_element_type=F32
    ).astype(BF16)
    for j in range(slabs):
        start = pl.multiple_of(j * seqs * owned + q * owned, owned)
        piece = numer[:, j * LANES : (j + 1) * LANES]
        payload[:, pl.ds(start, owned), :] = piece.reshape(shards, owned, LANES)

    row = lax.broadcasted_iota(jnp.int32, (PIECES, slots), 0)
    stacked = jnp.zeros((PIECES, slots), F32)
    for k, part in enumerate(pieces_of(top) + pieces_of(mass)):
        stacked = jnp.where(row == k, part, stacked)
    stats[pl.ds(pl.multiple_of(q * PIECES, PIECES), PIECES), :] = stacked

    peak = jnp.max(logits, axis=1, keepdims=True)
    raised = jnp.exp(logits - peak)
    mix = raised / jnp.sum(raised, axis=1, keepdims=True)
    mix = jnp.where(live, mix, 0.0).astype(BF16)
    per_seq = length // block
    for j in range(per_seq):
        mixes[peers[q * per_seq + j]] = mix[j * block : (j + 1) * block]

    @pl.when(q == last)
    def _():
        turned = stats[...].T
        lane = lax.broadcasted_iota(jnp.int32, (owned, LANES), 1)
        for d in range(shards):
            mine = turned[d * owned : (d + 1) * owned]
            mine = jnp.where(lane == LANES - 1, labels[d].astype(F32), mine)
            payload[d, stat_rows:, :] = mine.astype(BF16)


def dispatch(tokens, params, counts, peers, labels, shards):
    seqs, length, width = tokens.shape[1:]
    slots = params.shape[1]
    owned = slots // shards
    rows = width // LANES * seqs * owned + owned
    block = length * seqs // peers.shape[0]
    return pl.pallas_call(
        dispatch_kernel,
        grid_spec=pltpu.PrefetchScalarGridSpec(
            num_scalar_prefetch=3,
            grid=(seqs,),
            in_specs=[
                pl.BlockSpec((1, 1, length, width), lambda q, *_: (0, q, 0, 0)),
                pl.BlockSpec((width, slots), lambda q, *_: (0, 0)),
            ],
            out_specs=[
                pl.BlockSpec((shards, rows, LANES), lambda q, *_: (0, 0, 0)),
                pl.BlockSpec((shards, block, slots), lambda q, *_: (0, 0, 0)),
            ],
            scratch_shapes=[pltpu.VMEM((LANES, slots), F32)],
        ),
        out_shape=[
            jax.ShapeDtypeStruct((shards, rows, LANES), BF16),
            jax.ShapeDtypeStruct((shards, block, slots), BF16),
        ],
        name="dispatch",
    )(counts, peers, labels, tokens, params)


def expert_order(seqs, experts, per_expert, back):
    total = seqs * experts * per_expert
    here = lax.broadcasted_iota(jnp.int32, (total, total), 1 if back else 0)
    there = lax.broadcasted_iota(jnp.int32, (total, total), 0 if back else 1)
    expert = here // (seqs * per_expert)
    seq = here // per_expert % seqs
    rank = here % per_expert
    return (there == (seq * experts + expert) * per_expert + rank).astype(BF16)


def own_kernel(seqs, experts, received, result, labels):
    shards, rows, _ = received.shape
    owned = result.shape[1] // seqs
    stat_rows = rows - owned
    slabs = stat_rows // (seqs * owned)
    raw = received[:, stat_rows:, :].astype(F32)
    labels[...] = raw[:, 0, :]
    joined = raw + pltpu.roll(raw, LANES - 1, 2) + pltpu.roll(raw, LANES - 2, 2)
    top = jnp.max(joined, axis=0, keepdims=True)
    factor = jnp.exp(joined - top)
    mass = jnp.sum(joined * pltpu.roll(factor, 3, 2), axis=0, keepdims=True)
    scale = factor / pltpu.roll(mass, LANES - 3, 2)
    parts = []
    for q in range(seqs):
        totals = [jnp.zeros((owned, LANES), F32)] * slabs
        for s in range(shards):
            column = scale[s, :, q * PIECES : q * PIECES + 1]
            for j in range(slabs):
                start = (j * seqs + q) * owned
                totals[j] += received[s, start : start + owned, :].astype(F32) * column
        parts.append(jnp.concatenate(totals, axis=1))
    slot_in = jnp.concatenate(parts, axis=0).astype(BF16)
    order = expert_order(seqs, experts, owned // experts, False)
    ordered = jnp.dot(order, slot_in, preferred_element_type=F32).astype(BF16)
    for y in range(result.shape[0]):
        result[y] = ordered


def own_slots(received, seqs, experts, copies, owned):
    shards, rows, _ = received.shape
    width = (rows - owned) // (seqs * owned) * LANES
    return pl.pallas_call(
        functools.partial(own_kernel, seqs, experts),
        out_shape=[
            jax.ShapeDtypeStruct((copies, seqs * owned, width), BF16),
            jax.ShapeDtypeStruct((shards, LANES), F32),
        ],
        name="own_slots",
    )(received)


def gelu(x):
    return 0.5 * x * (1.0 + jnp.tanh(math.sqrt(2.0 / math.pi) * (x + 0.044715 * (x * x * x))))


def expert_kernel(own, other, first, second, own_out, other_out):
    copies, rows, width = own.shape
    half = copies * rows
    both = jnp.concatenate([own[...].reshape(half, width), other[...].reshape(half, width)], axis=0)
    hidden = gelu(jnp.dot(both, first[0], preferred_element_type=F32)).astype(BF16)
    result = jnp.dot(hidden, second[0], preferred_element_type=F32)
    own_out[...] = result[:half].reshape(copies, rows, width)
    other_out[...] = result[half:].reshape(copies, rows, width).astype(BF16)


def expert_layers(own, other, w_in, w_out):
    copies, rows, width = own.shape
    experts, _, hidden = w_in.shape
    each = rows // experts
    rows_spec = pl.BlockSpec((copies, each, width), lambda e: (0, e, 0))
    return pl.pallas_call(
        expert_kernel,
        grid=(experts,),
        in_specs=[
            rows_spec,
            rows_spec,
            pl.BlockSpec((1, width, hidden), lambda e: (e, 0, 0)),
            pl.BlockSpec((1, hidden, width), lambda e: (e, 0, 0)),
        ],
        out_specs=[rows_spec, rows_spec],
        out_shape=[
            jax.ShapeDtypeStruct(own.shape, F32),
            jax.ShapeDtypeStruct(own.shape, BF16),
        ],
        name="experts",
    )(own, other, w_in, w_out)


def collect_kernel(seqs, experts, partial, result):
    total = jnp.sum(partial[...].astype(F32), axis=0).astype(BF16)
    per_expert = total.shape[0] // (seqs * experts)
    order = expert_order(seqs, experts, per_expert, True)
    ordered = jnp.dot(order, total, preferred_element_type=F32).astype(BF16)
    for s in range(result.shape[0]):
        result[s] = ordered


def collect(partial, seqs, experts, shards):
    _, rows, width = partial.shape
    return pl.pallas_call(
        functools.partial(collect_kernel, seqs, experts),
        out_shape=jax.ShapeDtypeStruct((shards, rows, width), BF16),
        name="collect",
    )(partial)


def combine_kernel(source, seq, mix, outputs, result):
    shards, owned, width = outputs.shape
    slots = outputs[...].reshape(shards * owned, width)
    result[0, 0] = jnp.dot(mix[0], slots, preferred_element_type=F32).astype(BF16)


def combine(source, seq, mixes, outputs, seqs):
    shards, block, slots = mixes.shape
    width = outputs.shape[2]
    owned = outputs.shape[1] // seqs
    blocks = source.shape[0]
    return pl.pallas_call(
        combine_kernel,
        grid_spec=pltpu.PrefetchScalarGridSpec(
            num_scalar_prefetch=2,
            grid=(blocks,),
            in_specs=[
                pl.BlockSpec((1, block, slots), lambda b, source, seq: (source[b], 0, 0)),
                pl.BlockSpec((shards, owned, width), lambda b, source, seq: (0, seq[b], 0)),
            ],
            out_specs=pl.BlockSpec((1, 1, block, width), lambda b, source, seq: (0, b, 0, 0)),
        ),
        out_shape=jax.ShapeDtypeStruct((1, blocks, block, width), BF16),
        name="combine",
    )(source, seq, mixes, outputs)


def swapped(array):
    return lax.ppermute(array, "c", [(0, 1), (1, 0)])


def exchanged(array, axis):
    return lax.all_to_all(array, axis, split_axis=0, concat_axis=0, tiled=True)


def local(tokens, slot_params, dest, lengths, w_in, w_out):
    seqs, length = tokens.shape[1:3]
    held = dest.shape[1] * dest.shape[2]
    shards = lax.axis_size(EXPERT)
    experts = w_in.shape[0]
    owned = slot_params.shape[1] // shards
    counts = lengths[0] - lax.axis_index(EXPERT) * length
    targets = dest.reshape(held)
    peers = targets // held
    block_seq = jnp.arange(held, dtype=jnp.int32) // dest.shape[2]
    code = targets % held * seqs + block_seq + 1
    to_shard = jnp.arange(shards, dtype=jnp.int32)
    labels = jnp.sum(jnp.where(peers[None, :] == to_shard[:, None], code[None, :], 0), axis=1)

    payload, mixes = dispatch(tokens, slot_params, counts, peers, labels, shards)
    received = exchanged(payload, EXPERT)
    slot_in, tags = own_slots(received, seqs, experts, lax.axis_size("y"), owned)
    mixes, slot_in = lax.optimization_barrier((mixes, slot_in))
    arrived = exchanged(mixes, EXPERT)

    own = exchanged(slot_in, "y")
    own_out, other_out = expert_layers(own, swapped(own), w_in, w_out)
    partial = (own_out + swapped(other_out).astype(F32)).astype(BF16)
    outputs = exchanged(collect(exchanged(partial, "y"), seqs, experts, shards), EXPERT)

    found = tags[:, LANES - 1].astype(jnp.int32) - 1
    place = jnp.where(found >= 0, found // seqs, -1)
    match = place[None, :] == jnp.arange(held, dtype=jnp.int32)[:, None]
    source = jnp.sum(jnp.where(match, to_shard[None, :], 0), axis=1)
    seq = jnp.sum(jnp.where(match, found[None, :] % seqs, 0), axis=1)
    return combine(source, seq, arrived, outputs, seqs)


def solution(mesh):
    finer = Mesh(mesh.devices.reshape(4, 2, 4, 4), DP + EXPERT)
    in_specs = (
        P(DP, None, EXPERT, None),
        P(),
        P(DP, None, EXPERT),
        P(DP, None),
        P(EXPERT, None, DP),
        P(EXPERT, DP, None),
    )
    out_specs = P(DP, EXPERT, None, None)
    return jax.shard_map(local, mesh=finer, in_specs=in_specs, out_specs=out_specs, check_vma=False)
```

```python
import functools
import math

import jax
import jax.numpy as jnp
from jax import lax
from jax.experimental import pallas as pl
from jax.experimental.pallas import tpu as pltpu
from jax.sharding import Mesh
from jax.sharding import PartitionSpec as P

DP = ("y", "c")
EXPERT = ("z", "x")
LANES = 128
PIECES = 8
NO_TOKEN = -1e30
F32 = jnp.float32
BF16 = jnp.bfloat16


def pieces_of(value):
    high = value.astype(BF16).astype(F32)
    rest = value - high
    middle = rest.astype(BF16).astype(F32)
    return high, middle, rest - middle


def small(mebibytes):
    return pltpu.CompilerParams(vmem_limit_bytes=mebibytes * 1024 * 1024)


def in_vmem(*arrays):
    return [pltpu.with_memory_space_constraint(array, pltpu.VMEM) for array in arrays]


def in_hbm(*arrays):
    return [pltpu.with_memory_space_constraint(array, pltpu.HBM) for array in arrays]


ANYWHERE = pl.BlockSpec(memory_space=pl.ANY)
WHOLE = pl.BlockSpec(memory_space=pltpu.VMEM)
SCALARS = pl.BlockSpec(memory_space=pltpu.SMEM)


def dispatch_kernel(
    lengths, dest, shard, tokens, params, payload, mixes, stats, labels, blocks, sems
):
    q = pl.program_id(0)
    last = pl.num_programs(0) - 1
    feats = tokens[0, 0]
    length = feats.shape[0]
    shards = payload.shape[0]
    slots = params.shape[1]
    owned = slots // shards
    slabs = feats.shape[1] // LANES
    stat_rows = payload.shape[1] - owned
    seqs = stat_rows // (slabs * owned)
    block = mixes.shape[1]
    per_seq = length // block
    held = per_seq * seqs

    @pl.when(q == 0)
    def _():
        stats[...] = jnp.zeros(stats.shape, stats.dtype)
        for d in range(shards):
            labels[d] = 0
        for j in range(per_seq):
            for k in range(seqs):
                target = dest[j, k]
                labels[lax.div(target, held)] = lax.rem(target, held) * seqs + k + 1

    logits = jnp.dot(feats, params[...], preferred_element_type=F32)
    count = lengths[0, q] - shard[0] * length
    live = lax.broadcasted_iota(jnp.int32, (length, 1), 0) < count
    masked = jnp.where(live, logits, NO_TOKEN)
    top = jnp.max(masked, axis=0, keepdims=True)
    weight = jnp.where(live, jnp.exp(masked - top), 0.0)
    mass = jnp.sum(weight, axis=0, keepdims=True)
    numer = lax.dot_general(
        weight.astype(BF16), feats, (((0,), (0,)), ((), ())), preferred_element_type=F32
    ).astype(BF16)
    for j in range(slabs):
        start = pl.multiple_of(j * seqs * owned + q * owned, owned)
        piece = numer[:, j * LANES : (j + 1) * LANES]
        payload[:, pl.ds(start, owned), :] = piece.reshape(shards, owned, LANES)

    row = lax.broadcasted_iota(jnp.int32, (PIECES, slots), 0)
    stacked = jnp.zeros((PIECES, slots), F32)
    for k, part in enumerate(pieces_of(top) + pieces_of(mass)):
        stacked = jnp.where(row == k, part, stacked)
    stats[pl.ds(pl.multiple_of(q * PIECES, PIECES), PIECES), :] = stacked

    peak = jnp.max(logits, axis=1, keepdims=True)
    raised = jnp.exp(logits - peak)
    mix = raised * (1.0 / jnp.sum(raised, axis=1, keepdims=True))
    mix = jnp.where(live, mix, 0.0).astype(BF16)
    blocks[q] = mix

    def send(step, j):
        place = mixes.at[lax.div(dest[j, step], held)]
        return pltpu.make_async_copy(
            blocks.at[step, pl.ds(j * block, block)], place, sems.at[step, j]
        )

    for j in range(per_seq):
        send(q, j).start()

    @pl.when(q == last)
    def _():
        turned = stats[...].T
        lane = lax.broadcasted_iota(jnp.int32, (owned, LANES), 1)
        for d in range(shards):
            mine = turned[d * owned : (d + 1) * owned]
            mine = jnp.where(lane == LANES - 1, labels[d].astype(F32), mine)
            payload[d, stat_rows:, :] = mine.astype(BF16)
        for k in range(seqs):
            for j in range(per_seq):
                send(k, j).wait()


def dispatch(tokens, params, lengths, dest, shard, shards):
    seqs, length, width = tokens.shape[1:]
    slots = params.shape[1]
    owned = slots // shards
    rows = width // LANES * seqs * owned + owned
    block = length // dest.shape[0]
    return pl.pallas_call(
        dispatch_kernel,
        grid=(seqs,),
        in_specs=[
            SCALARS,
            SCALARS,
            SCALARS,
            pl.BlockSpec((1, 1, length, width), lambda q: (0, q, 0, 0)),
            pl.BlockSpec((width, slots), lambda q: (0, 0)),
        ],
        out_specs=[WHOLE, ANYWHERE],
        scratch_shapes=[
            pltpu.VMEM((LANES, slots), F32),
            pltpu.SMEM((shards,), jnp.int32),
            pltpu.VMEM((seqs, length, slots), BF16),
            pltpu.SemaphoreType.DMA((seqs, dest.shape[0])),
        ],
        out_shape=[
            pltpu.VMEM((shards, rows, LANES), BF16),
            pltpu.HBM((shards, block, slots), BF16),
        ],
        compiler_params=small(16),
        name="dispatch",
    )(*in_hbm(lengths, dest), shard, *in_hbm(tokens, params))


def expert_order(seqs, experts, per_expert, back):
    total = seqs * experts * per_expert
    here = lax.broadcasted_iota(jnp.int32, (total, total), 1 if back else 0)
    there = lax.broadcasted_iota(jnp.int32, (total, total), 0 if back else 1)
    expert = here // (seqs * per_expert)
    seq = here // per_expert % seqs
    rank = here % per_expert
    return (there == (seq * experts + expert) * per_expert + rank).astype(BF16)


def own_kernel(seqs, experts, received, result, labels):
    shards, rows, _ = received.shape
    owned = result.shape[0] // seqs
    stat_rows = rows - owned
    slabs = stat_rows // (seqs * owned)
    raw = received[:, stat_rows:, :].astype(F32)
    labels[...] = raw[:, 0, :]
    joined = raw + pltpu.roll(raw, LANES - 1, 2) + pltpu.roll(raw, LANES - 2, 2)
    top = jnp.max(joined, axis=0, keepdims=True)
    factor = jnp.exp(joined - top)
    mass = jnp.sum(joined * pltpu.roll(factor, 3, 2), axis=0, keepdims=True)
    scale = factor / pltpu.roll(mass, LANES - 3, 2)
    parts = []
    for q in range(seqs):
        totals = [jnp.zeros((owned, LANES), F32)] * slabs
        for s in range(shards):
            column = scale[s, :, q * PIECES : q * PIECES + 1]
            for j in range(slabs):
                start = (j * seqs + q) * owned
                totals[j] += received[s, start : start + owned, :].astype(F32) * column
        parts.append(jnp.concatenate(totals, axis=1))
    slot_in = jnp.concatenate(parts, axis=0).astype(BF16)
    order = expert_order(seqs, experts, owned // experts, False)
    ordered = jnp.dot(order, slot_in, preferred_element_type=F32).astype(BF16)
    result[...] = ordered


def own_slots(received, seqs, experts, owned):
    shards, rows, _ = received.shape
    width = (rows - owned) // (seqs * owned) * LANES
    return pl.pallas_call(
        functools.partial(own_kernel, seqs, experts),
        in_specs=[WHOLE],
        out_specs=[WHOLE, WHOLE],
        out_shape=[
            pltpu.VMEM((seqs * owned, width), BF16),
            jax.ShapeDtypeStruct((shards, LANES), F32),
        ],
        compiler_params=small(8),
        name="own_slots",
    )(*in_vmem(received))


def gelu(x):
    return 0.5 * x * (1.0 + jnp.tanh(math.sqrt(2.0 / math.pi) * (x + 0.044715 * (x * x * x))))


def expert_kernel(count, *refs):
    rows = refs[:count]
    first_far, second_far, own_out, other_out, first, second, sems = refs[count:]
    experts = first.shape[0]
    each = rows[0].shape[0] // experts
    half = count // 2
    loads = []
    for e in range(experts):
        loads.append(pltpu.make_async_copy(first_far.at[e], first.at[e], sems.at[0, e]))
        loads.append(pltpu.make_async_copy(second_far.at[e], second.at[e], sems.at[1, e]))
    for load in loads:
        load.start()
    for e in range(experts):
        span = slice(e * each, (e + 1) * each)
        both = jnp.concatenate([ref[span, :] for ref in rows], axis=0)
        loads[2 * e].wait()
        hidden = gelu(jnp.dot(both, first[e], preferred_element_type=F32)).astype(BF16)
        loads[2 * e + 1].wait()
        result = jnp.dot(hidden, second[e], preferred_element_type=F32)
        for k in range(half):
            own_out[k, span, :] = result[k * each : (k + 1) * each]
            other = result[(half + k) * each : (half + k + 1) * each]
            other_out[k, span, :] = other.astype(BF16)


def expert_layers(own, other, first, second):
    shape = (len(own), *own[0].shape)
    count = len(own) + len(other)
    return pl.pallas_call(
        functools.partial(expert_kernel, count),
        in_specs=[WHOLE] * count + [ANYWHERE, ANYWHERE],
        out_specs=[WHOLE, WHOLE],
        out_shape=[pltpu.VMEM(shape, F32), pltpu.VMEM(shape, BF16)],
        scratch_shapes=[
            pltpu.VMEM(first.shape, first.dtype),
            pltpu.VMEM(second.shape, second.dtype),
            pltpu.SemaphoreType.DMA((2, first.shape[0])),
        ],
        compiler_params=small(24),
        name="experts",
    )(*in_vmem(*own, *other), *in_hbm(first, second))


def join_kernel(own, other, kept, *sent):
    kept[...] = own[0] + other[0].astype(F32)
    for k, ref in enumerate(sent):
        ref[...] = (own[k + 1] + other[k + 1].astype(F32)).astype(BF16)


def join(own, other):
    copies, rows, width = own.shape
    return pl.pallas_call(
        join_kernel,
        in_specs=[WHOLE, WHOLE],
        out_specs=[WHOLE] * copies,
        out_shape=[pltpu.VMEM((rows, width), F32)] + [pltpu.VMEM((rows, width), BF16)] * (copies - 1),
        compiler_params=small(4),
        name="join",
    )(*in_vmem(own, other))


def collect_kernel(seqs, experts, kept, *refs):
    result, ordered, sems = refs[-3:]
    total = kept[...]
    for ref in refs[:-3]:
        total += ref[...].astype(F32)
    total = total.astype(BF16)
    per_expert = total.shape[0] // (seqs * experts)
    order = expert_order(seqs, experts, per_expert, True)
    ordered[...] = jnp.dot(order, total, preferred_element_type=F32).astype(BF16)
    copies = [
        pltpu.make_async_copy(ordered, result.at[s], sems.at[s]) for s in range(result.shape[0])
    ]
    for copy in copies:
        copy.start()
    for copy in copies:
        copy.wait()


def collect(kept, parts, seqs, experts, shards):
    rows, width = kept.shape
    return pl.pallas_call(
        functools.partial(collect_kernel, seqs, experts),
        in_specs=[WHOLE] * (1 + len(parts)),
        out_specs=ANYWHERE,
        out_shape=pltpu.HBM((shards, rows, width), BF16),
        scratch_shapes=[pltpu.VMEM((rows, width), BF16), pltpu.SemaphoreType.DMA((shards,))],
        compiler_params=small(4),
        name="collect",
    )(*in_vmem(kept, *parts))


def combine_kernel(source, seq, mix, outputs, result):
    b = pl.program_id(0)
    shards, rows, width = outputs.shape
    owned = mix.shape[2] // shards
    start = pl.multiple_of(seq[b] * owned, owned)
    slots = outputs[:, pl.ds(start, owned), :].reshape(shards * owned, width)
    result[0, 0] = jnp.dot(mix[source[b]], slots, preferred_element_type=F32).astype(BF16)


def combine(source, seq, mixes, outputs):
    _, block, _ = mixes.shape
    width = outputs.shape[2]
    blocks = source.shape[0]
    return pl.pallas_call(
        combine_kernel,
        grid=(blocks,),
        in_specs=[SCALARS, SCALARS, WHOLE, WHOLE],
        out_specs=pl.BlockSpec((1, 1, block, width), lambda b: (0, b, 0, 0)),
        out_shape=jax.ShapeDtypeStruct((1, blocks, block, width), BF16),
        compiler_params=small(8),
        name="combine",
    )(source, seq, *in_vmem(mixes, outputs))


def swapped(array):
    return lax.ppermute(array, "c", [(0, 1), (1, 0)])


def exchanged(array, axis):
    return lax.all_to_all(array, axis, split_axis=0, concat_axis=0, tiled=True)


def moved(array, axis, step):
    size = lax.axis_size(axis)
    return lax.ppermute(array, axis, [(i, (i + step) % size) for i in range(size)])


def local(tokens, slot_params, dest, lengths, w_in, w_out):
    seqs, _ = tokens.shape[1:3]
    held = dest.shape[1] * dest.shape[2]
    shards = lax.axis_size(EXPERT)
    experts = w_in.shape[0]
    owned = slot_params.shape[1] // shards
    planes = lax.axis_size("y")
    shard = lax.axis_index(EXPERT).reshape(1)
    table = dest[0].T

    payload, mixes = dispatch(tokens, slot_params, lengths, table, shard, shards)
    received = exchanged(payload, EXPERT)
    slot_in, tags = own_slots(received, seqs, experts, owned)
    mixes, slot_in = lax.optimization_barrier((mixes, slot_in))
    arrived = exchanged(mixes, EXPERT)

    own = [slot_in] + [moved(slot_in, "y", k) for k in range(1, planes)]
    other = [swapped(piece) for piece in own]
    own_out, other_out = expert_layers(own, other, w_in, w_out)
    kept, *sent = join(own_out, swapped(other_out))
    parts = [moved(piece, "y", -k - 1) for k, piece in enumerate(sent)]
    found = tags[:, LANES - 1].astype(jnp.int32) - 1
    place = jnp.where(found >= 0, found // seqs, -1)
    match = place[None, :] == jnp.arange(held, dtype=jnp.int32)[:, None]
    to_shard = jnp.arange(shards, dtype=jnp.int32)
    source = jnp.sum(jnp.where(match, to_shard[None, :], 0), axis=1)
    seq = jnp.sum(jnp.where(match, found[None, :] % seqs, 0), axis=1)
    slot_out = collect(kept, parts, seqs, experts, shards)
    slot_out, source, seq = lax.optimization_barrier((slot_out, source, seq))
    return combine(source, seq, arrived, exchanged(slot_out, EXPERT))


def solution(mesh):
    finer = Mesh(mesh.devices.reshape(4, 2, 4, 4), DP + EXPERT)
    in_specs = (
        P(DP, None, EXPERT, None),
        P(),
        P(DP, None, EXPERT),
        P(DP, None),
        P(EXPERT, None, DP),
        P(EXPERT, DP, None),
    )
    out_specs = P(DP, EXPERT, None, None)
    return jax.shard_map(local, mesh=finer, in_specs=in_specs, out_specs=out_specs, check_vma=False)
```

```python
import functools
import math

import jax
import jax.numpy as jnp
from jax import lax
from jax.experimental import pallas as pl
from jax.experimental.pallas import tpu as pltpu
from jax.sharding import Mesh
from jax.sharding import PartitionSpec as P

DP = ("y", "c")
EXPERT = ("z", "x")
LANES = 128
PIECES = 8
TAGS = 64
NO_TOKEN = -1e30
F32 = jnp.float32
BF16 = jnp.bfloat16


def pieces_of(value):
    high = value.astype(BF16).astype(F32)
    rest = value - high
    middle = rest.astype(BF16).astype(F32)
    return high, middle, rest - middle


def small(mebibytes):
    return pltpu.CompilerParams(vmem_limit_bytes=mebibytes * 1024 * 1024)


def in_vmem(*arrays):
    return [pltpu.with_memory_space_constraint(array, pltpu.VMEM) for array in arrays]


def in_hbm(*arrays):
    return [pltpu.with_memory_space_constraint(array, pltpu.HBM) for array in arrays]


ANYWHERE = pl.BlockSpec(memory_space=pl.ANY)
WHOLE = pl.BlockSpec(memory_space=pltpu.VMEM)
SCALARS = pl.BlockSpec(memory_space=pltpu.SMEM)


def line_order(total, owned, swap):
    side = math.isqrt(total // owned)
    column = lax.broadcasted_iota(jnp.int32, (total, total), 1)
    place = column // owned
    shard = jnp.where(swap, place % side * side + place // side, place)
    source = shard * owned + column % owned
    return (lax.broadcasted_iota(jnp.int32, (total, total), 0) == source).astype(BF16)


def dispatch_kernel(lengths, dest, place, tokens, params, *refs):
    side = 4
    parts = refs[:side]
    mixes, order, sums, turned, stats, labels, blocks, sems = refs[side:]
    q = pl.program_id(0)
    last = pl.num_programs(0) - 1
    shard, core, line = place[0], place[1], place[2]
    feats = tokens[0, 0]
    length = feats.shape[0]
    slots = params.shape[1]
    owned = slots // (side * side)
    slabs = feats.shape[1] // LANES
    stat_rows = parts[0].shape[1] - owned
    seqs = stat_rows // (slabs * owned)
    block = mixes.shape[1]
    per_seq = length // block
    held = per_seq * seqs
    group = side * owned

    @pl.when(q == 0)
    def _():
        sorting = line_order(slots, owned, core == 1)
        order[...] = jnp.dot(params[...], sorting, preferred_element_type=F32).astype(BF16)
        stats[...] = jnp.zeros(stats.shape, stats.dtype)
        for d in range(side * side):
            labels[d] = 0
        for j in range(per_seq):
            for k in range(seqs):
                target = dest[j, k]
                labels[lax.div(target, held)] = lax.rem(target, held) * seqs + k + 1

    logits = jnp.dot(feats, order[...], preferred_element_type=F32)
    count = lengths[0, q] - shard * length
    live = lax.broadcasted_iota(jnp.int32, (length, 1), 0) < count
    masked = jnp.where(live, logits, NO_TOKEN)
    top = jnp.max(masked, axis=0, keepdims=True)
    weight = jnp.where(live, jnp.exp(masked - top), 0.0)
    mass = jnp.sum(weight, axis=0, keepdims=True)
    sums[...] = lax.dot_general(
        weight.astype(BF16), feats, (((0,), (0,)), ((), ())), preferred_element_type=F32
    ).astype(BF16)
    for k, part in enumerate(parts):
        first = pl.multiple_of(lax.rem(line + k, side) * group, group)
        numer = sums[pl.ds(first, group), :]
        for j in range(slabs):
            start = pl.multiple_of((j * seqs + q) * owned, owned)
            piece = numer[:, j * LANES : (j + 1) * LANES]
            part[:, pl.ds(start, owned), :] = piece.reshape(side, owned, LANES)

    row = lax.broadcasted_iota(jnp.int32, (PIECES, slots), 0)
    stacked = jnp.zeros((PIECES, slots), F32)
    for k, piece in enumerate(pieces_of(top) + pieces_of(mass)):
        stacked = jnp.where(row == k, piece, stacked)
    stats[pl.ds(pl.multiple_of(q * PIECES, PIECES), PIECES), :] = stacked

    peak = jnp.max(logits, axis=1, keepdims=True)
    raised = jnp.exp(logits - peak)
    mix = raised * (1.0 / jnp.sum(raised, axis=1, keepdims=True))
    mix = jnp.where(live, mix, 0.0).astype(BF16)
    blocks[q] = mix

    def send(step, j):
        target = mixes.at[lax.div(dest[j, step], held)]
        return pltpu.make_async_copy(
            blocks.at[step, pl.ds(j * block, block)], target, sems.at[step, j]
        )

    for j in range(per_seq):
        send(q, j).start()

    @pl.when(q == last)
    def _():
        turned[...] = stats[...].T
        lane = lax.broadcasted_iota(jnp.int32, (owned, LANES), 1)
        for k, part in enumerate(parts):
            ahead = lax.rem(line + k, side)
            mine = turned[pl.ds(pl.multiple_of(ahead * group, group), group), :]
            for n in range(side):
                target = jnp.where(core == 1, n * side + ahead, ahead * side + n)
                tag = labels[target].astype(F32)
                piece = jnp.where(lane == TAGS + line, tag, mine[n * owned : (n + 1) * owned])
                part[n, stat_rows:, :] = piece.astype(BF16)
        for k in range(seqs):
            for j in range(per_seq):
                send(k, j).wait()


def dispatch(tokens, params, lengths, dest, place, side):
    seqs, length, width = tokens.shape[1:]
    slots = params.shape[1]
    owned = slots // (side * side)
    rows = width // LANES * seqs * owned + owned
    per_seq = dest.shape[0]
    block = length // per_seq
    return pl.pallas_call(
        dispatch_kernel,
        grid=(seqs,),
        in_specs=[
            SCALARS,
            SCALARS,
            SCALARS,
            pl.BlockSpec((1, 1, length, width), lambda q: (0, q, 0, 0)),
            pl.BlockSpec((width, slots), lambda q: (0, 0)),
        ],
        out_specs=[WHOLE] * side + [ANYWHERE],
        scratch_shapes=[
            pltpu.VMEM((width, slots), BF16),
            pltpu.VMEM((slots, width), BF16),
            pltpu.VMEM((slots, LANES), F32),
            pltpu.VMEM((LANES, slots), F32),
            pltpu.SMEM((side * side,), jnp.int32),
            pltpu.VMEM((seqs, length, slots), BF16),
            pltpu.SemaphoreType.DMA((seqs, per_seq)),
        ],
        out_shape=[pltpu.VMEM((side, rows, LANES), BF16)] * side
        + [pltpu.HBM((side * side, block, slots), BF16)],
        compiler_params=small(16),
        name="dispatch",
    )(*in_hbm(lengths, dest), place, *in_hbm(tokens, params))


def joined_stats(raws):
    tops = [raw + pltpu.roll(raw, LANES - 1, 1) + pltpu.roll(raw, LANES - 2, 1) for raw in raws]
    top = functools.reduce(jnp.maximum, tops)
    factors = [jnp.exp(each - top) for each in tops]
    mass = sum(each * pltpu.roll(factor, 3, 1) for each, factor in zip(tops, factors))
    return top, mass, factors


def merge_kernel(place, *refs):
    side = 4
    sources, results = refs[:side], refs[side:]
    rows = sources[0].shape[1]
    owned = 16
    seqs = 4
    stat_rows = rows - owned
    slabs = stat_rows // (seqs * owned)
    lane = lax.broadcasted_iota(jnp.int32, (owned, LANES), 1)
    for k, result in enumerate(results):
        ahead = lax.rem(place[3] + k, side)
        raws = [source[ahead, stat_rows:, :].astype(F32) for source in sources]
        top, mass, factors = joined_stats(raws)
        stat = jnp.where(lane >= TAGS, sum(raws), 0.0)
        for value, first in ((top, 0), (mass, 3)):
            for n, piece in enumerate(pieces_of(value)):
                spread = pltpu.roll(piece, n, 1) if n else piece
                stat = jnp.where((lane < TAGS) & (lane % PIECES == first + n), spread, stat)
        result[stat_rows:, :] = stat.astype(BF16)
        for q in range(seqs):
            columns = [factor[:, q * PIECES : q * PIECES + 1] for factor in factors]
            for j in range(slabs):
                start = (j * seqs + q) * owned
                total = sum(
                    source[ahead, start : start + owned, :].astype(F32) * column
                    for source, column in zip(sources, columns)
                )
                result[start : start + owned, :] = total.astype(BF16)


def merge(place, parts):
    side, rows, _ = parts[0].shape
    return pl.pallas_call(
        merge_kernel,
        in_specs=[SCALARS] + [WHOLE] * side,
        out_specs=[WHOLE] * side,
        out_shape=[pltpu.VMEM((rows, LANES), BF16)] * side,
        compiler_params=small(4),
        name="merge",
    )(place, *in_vmem(*parts))


def expert_order(seqs, experts, per_expert, back):
    total = seqs * experts * per_expert
    here = lax.broadcasted_iota(jnp.int32, (total, total), 1 if back else 0)
    there = lax.broadcasted_iota(jnp.int32, (total, total), 0 if back else 1)
    expert = here // (seqs * per_expert)
    seq = here // per_expert % seqs
    rank = here % per_expert
    return (there == (seq * experts + expert) * per_expert + rank).astype(BF16)


def own_kernel(seqs, experts, *refs):
    received, (result, labels) = refs[:-2], refs[-2:]
    rows, _ = received[0].shape
    owned = result.shape[0] // seqs
    stat_rows = rows - owned
    slabs = stat_rows // (seqs * owned)
    raws = [source[stat_rows:, :].astype(F32) for source in received]
    for k, raw in enumerate(raws):
        labels[k : k + 1, :] = raw[:1]
    _, mass, factors = joined_stats(raws)
    mass = pltpu.roll(mass, LANES - 3, 1)
    parts = []
    for q in range(seqs):
        totals = [jnp.zeros((owned, LANES), F32)] * slabs
        for source, factor in zip(received, factors):
            column = (factor / mass)[:, q * PIECES : q * PIECES + 1]
            for j in range(slabs):
                start = (j * seqs + q) * owned
                totals[j] += source[start : start + owned, :].astype(F32) * column
        parts.append(jnp.concatenate(totals, axis=1))
    slot_in = jnp.concatenate(parts, axis=0).astype(BF16)
    order = expert_order(seqs, experts, owned // experts, False)
    ordered = jnp.dot(order, slot_in, preferred_element_type=F32).astype(BF16)
    result[...] = ordered


def own_slots(received, seqs, experts, owned):
    rows, _ = received[0].shape
    width = (rows - owned) // (seqs * owned) * LANES
    return pl.pallas_call(
        functools.partial(own_kernel, seqs, experts),
        in_specs=[WHOLE] * len(received),
        out_specs=[WHOLE, WHOLE],
        out_shape=[
            pltpu.VMEM((seqs * owned, width), BF16),
            jax.ShapeDtypeStruct((len(received), LANES), F32),
        ],
        compiler_params=small(4),
        name="own_slots",
    )(*in_vmem(*received))


def gelu(x):
    return 0.5 * x * (1.0 + jnp.tanh(math.sqrt(2.0 / math.pi) * (x + 0.044715 * (x * x * x))))


def expert_kernel(count, *refs):
    rows = refs[:count]
    first_far, second_far, own_out, other_out, first, second, sems = refs[count:]
    experts = first.shape[0]
    each = rows[0].shape[0] // experts
    half = count // 2
    loads = []
    for e in range(experts):
        loads.append(pltpu.make_async_copy(first_far.at[e], first.at[e], sems.at[0, e]))
        loads.append(pltpu.make_async_copy(second_far.at[e], second.at[e], sems.at[1, e]))
    for load in loads:
        load.start()
    for e in range(experts):
        span = slice(e * each, (e + 1) * each)
        both = jnp.concatenate([ref[span, :] for ref in rows], axis=0)
        loads[2 * e].wait()
        hidden = gelu(jnp.dot(both, first[e], preferred_element_type=F32)).astype(BF16)
        loads[2 * e + 1].wait()
        result = jnp.dot(hidden, second[e], preferred_element_type=F32)
        for k in range(half):
            own_out[k, span, :] = result[k * each : (k + 1) * each]
            other = result[(half + k) * each : (half + k + 1) * each]
            other_out[k, span, :] = other.astype(BF16)


def expert_layers(own, other, first, second):
    shape = (len(own), *own[0].shape)
    count = len(own) + len(other)
    return pl.pallas_call(
        functools.partial(expert_kernel, count),
        in_specs=[WHOLE] * count + [ANYWHERE, ANYWHERE],
        out_specs=[WHOLE, WHOLE],
        out_shape=[pltpu.VMEM(shape, F32), pltpu.VMEM(shape, BF16)],
        scratch_shapes=[
            pltpu.VMEM(first.shape, first.dtype),
            pltpu.VMEM(second.shape, second.dtype),
            pltpu.SemaphoreType.DMA((2, first.shape[0])),
        ],
        compiler_params=small(24),
        name="experts",
    )(*in_vmem(*own, *other), *in_hbm(first, second))


def join_kernel(own, other, kept, *sent):
    kept[...] = own[0] + other[0].astype(F32)
    for k, ref in enumerate(sent):
        ref[...] = (own[k + 1] + other[k + 1].astype(F32)).astype(BF16)


def join(own, other):
    copies, rows, width = own.shape
    return pl.pallas_call(
        join_kernel,
        in_specs=[WHOLE, WHOLE],
        out_specs=[WHOLE] * copies,
        out_shape=[pltpu.VMEM((rows, width), F32)] + [pltpu.VMEM((rows, width), BF16)] * (copies - 1),
        compiler_params=small(4),
        name="join",
    )(*in_vmem(own, other))


def collect_kernel(seqs, experts, kept, *refs):
    result = refs[-1]
    total = kept[...]
    for ref in refs[:-1]:
        total += ref[...].astype(F32)
    total = total.astype(BF16)
    per_expert = total.shape[0] // (seqs * experts)
    order = expert_order(seqs, experts, per_expert, True)
    result[...] = jnp.dot(order, total, preferred_element_type=F32).astype(BF16)


def collect(kept, parts, seqs, experts):
    return pl.pallas_call(
        functools.partial(collect_kernel, seqs, experts),
        in_specs=[WHOLE] * (1 + len(parts)),
        out_specs=WHOLE,
        out_shape=pltpu.VMEM(kept.shape, BF16),
        compiler_params=small(4),
        name="collect",
    )(*in_vmem(kept, *parts))


def stack_kernel(place, *refs):
    result = refs[-1]
    side = result.shape[0]
    for k, ref in enumerate(refs[:-1]):
        result[lax.rem(place[2] + side - k, side)] = ref[...]


def stack(place, pieces):
    return pl.pallas_call(
        stack_kernel,
        in_specs=[SCALARS] + [WHOLE] * len(pieces),
        out_specs=WHOLE,
        out_shape=pltpu.VMEM((len(pieces), *pieces[0].shape), BF16),
        compiler_params=small(4),
        name="stack",
    )(place, *in_vmem(*pieces))


def combine_kernel(source, seq, place, mix, *refs):
    b = pl.program_id(0)
    lines, (result, slots) = refs[:-2], refs[-2:]
    side, rows, _ = lines[0].shape
    seqs = slots.shape[0]
    owned = rows // seqs

    @pl.when(b == 0)
    def _():
        for k, line in enumerate(lines):
            column = lax.rem(place[3] + side - k, side) * owned
            for f in range(side):
                start = pl.multiple_of(f * side * owned + column, owned)
                for q in range(seqs):
                    slots[q, pl.ds(start, owned), :] = line[f, q * owned : (q + 1) * owned, :]

    chosen = slots[seq[b]]
    result[0, 0] = jnp.dot(mix[source[b]], chosen, preferred_element_type=F32).astype(BF16)


def combine(source, seq, place, mixes, lines, seqs):
    _, block, slots = mixes.shape
    width = lines[0].shape[2]
    blocks = source.shape[0]
    return pl.pallas_call(
        combine_kernel,
        grid=(blocks,),
        in_specs=[SCALARS, SCALARS, SCALARS] + [WHOLE] * (1 + len(lines)),
        out_specs=pl.BlockSpec((1, 1, block, width), lambda b: (0, b, 0, 0)),
        out_shape=jax.ShapeDtypeStruct((1, blocks, block, width), BF16),
        scratch_shapes=[pltpu.VMEM((seqs, slots, width), BF16)],
        compiler_params=small(12),
        name="combine",
    )(source, seq, place, *in_vmem(mixes, *lines))


def swapped(array):
    return lax.ppermute(array, "c", [(0, 1), (1, 0)])


def exchanged(array, axis):
    return lax.all_to_all(array, axis, split_axis=0, concat_axis=0, tiled=True)


def moved(array, axis, step):
    size = lax.axis_size(axis)
    return lax.ppermute(array, axis, [(i, (i + step) % size) for i in range(size)])


def along(array, first, step):
    side = lax.axis_size("z")
    pairs = []
    for c in range(lax.axis_size("c")):
        for z in range(side):
            for x in range(side):
                in_z = first == (c == 0)
                to_z, to_x = ((z + step) % side, x) if in_z else (z, (x + step) % side)
                pairs.append(((c * side + z) * side + x, (c * side + to_z) * side + to_x))
    return lax.ppermute(array, ("c",) + EXPERT, pairs)


def local(tokens, slot_params, dest, lengths, w_in, w_out):
    seqs, _ = tokens.shape[1:3]
    held = dest.shape[1] * dest.shape[2]
    side = lax.axis_size("z")
    experts = w_in.shape[0]
    owned = slot_params.shape[1] // (side * side)
    planes = lax.axis_size("y")
    z, x, core = lax.axis_index("z"), lax.axis_index("x"), lax.axis_index("c")
    swap = core == 1
    place = jnp.stack([z * side + x, core, jnp.where(swap, x, z), jnp.where(swap, z, x)])
    table = dest[0].T

    *parts, mixes = dispatch(tokens, slot_params, lengths, table, place, side)
    steps = range(1, side)
    parts = merge(place, [parts[0]] + [along(parts[k], True, k) for k in steps])
    received = [parts[0]] + [along(parts[k], False, k) for k in steps]
    slot_in, tags = own_slots(received, seqs, experts, owned)
    mixes, slot_in = lax.optimization_barrier((mixes, slot_in))
    arrived = exchanged(mixes, EXPERT)

    own = [slot_in] + [moved(slot_in, "y", k) for k in range(1, planes)]
    other = [swapped(piece) for piece in own]
    own_out, other_out = expert_layers(own, other, w_in, w_out)
    kept, *sent = join(own_out, swapped(other_out))
    parts = [moved(piece, "y", -k - 1) for k, piece in enumerate(sent)]
    slot_out = collect(kept, parts, seqs, experts)

    found = tags[:, TAGS : TAGS + side].astype(jnp.int32) - 1
    line = jnp.arange(side, dtype=jnp.int32)[None, :]
    across = (place[3] - jnp.arange(side, dtype=jnp.int32)[:, None]) % side
    shard = jnp.where(swap, across * side + line, line * side + across).reshape(-1)
    found = found.reshape(-1)
    block = jnp.where(found >= 0, found // seqs, -1)
    match = block[None, :] == jnp.arange(held, dtype=jnp.int32)[:, None]
    source = jnp.sum(jnp.where(match, shard[None, :], 0), axis=1)
    seq = jnp.sum(jnp.where(match, found[None, :] % seqs, 0), axis=1)

    pieces = stack(place, [slot_out] + [along(slot_out, True, k) for k in steps])
    lines = [pieces] + [along(pieces, False, k) for k in steps]
    return combine(source, seq, place, arrived, lines, seqs)


def solution(mesh):
    finer = Mesh(mesh.devices.reshape(4, 2, 4, 4), DP + EXPERT)
    in_specs = (
        P(DP, None, EXPERT, None),
        P(),
        P(DP, None, EXPERT),
        P(DP, None),
        P(EXPERT, None, DP),
        P(EXPERT, DP, None),
    )
    out_specs = P(DP, EXPERT, None, None)
    return jax.shard_map(local, mesh=finer, in_specs=in_specs, out_specs=out_specs, check_vma=False)
```

```python
import functools
import math

import jax
import jax.numpy as jnp
from jax import lax
from jax.experimental import pallas as pl
from jax.experimental.pallas import tpu as pltpu
from jax.sharding import Mesh
from jax.sharding import PartitionSpec as P


DP = ("y", "c")
EXPERT = ("z", "x")
LANES = 128
PIECES = 8
TAGS = 64
NO_TOKEN = -1e30
F32 = jnp.float32
BF16 = jnp.bfloat16


def pieces_of(value):
    high = value.astype(BF16).astype(F32)
    rest = value - high
    middle = rest.astype(BF16).astype(F32)
    return high, middle, rest - middle


def small(mebibytes):
    return pltpu.CompilerParams(vmem_limit_bytes=mebibytes * 1024 * 1024)


def in_vmem(*arrays):
    return [pltpu.with_memory_space_constraint(array, pltpu.VMEM) for array in arrays]


def in_hbm(*arrays):
    return [pltpu.with_memory_space_constraint(array, pltpu.HBM) for array in arrays]


ANYWHERE = pl.BlockSpec(memory_space=pl.ANY)
WHOLE = pl.BlockSpec(memory_space=pltpu.VMEM)
SCALARS = pl.BlockSpec(memory_space=pltpu.SMEM)


def line_order(total, owned, swap):
    side = math.isqrt(total // owned)
    column = lax.broadcasted_iota(jnp.int32, (total, total), 1)
    place = column // owned
    shard = jnp.where(swap, place % side * side + place // side, place)
    source = shard * owned + column % owned
    return (lax.broadcasted_iota(jnp.int32, (total, total), 0) == source).astype(BF16)


def dispatch_kernel(lengths, dest, place, tokens, params, *refs):
    side = 4
    parts = refs[:side]
    mixes, plain, order, held_tokens, sums, turned, stats, labels, blocks, loads, sems = refs[side:]
    shard, core, line = place[0], place[1], place[2]
    _, seqs, length, width = tokens.shape
    slots = params.shape[1]
    owned = slots // (side * side)
    slabs = width // LANES
    stat_rows = parts[0].shape[1] - owned
    block = mixes.shape[1]
    per_seq = length // block
    held = per_seq * seqs
    group = side * owned

    first_load = pltpu.make_async_copy(params, plain, loads.at[seqs])
    first_load.start()
    arrivals = []
    for q in range(seqs):
        arrivals.append(pltpu.make_async_copy(tokens.at[0, q], held_tokens.at[q], loads.at[q]))
        arrivals[-1].start()
    stats[...] = jnp.zeros(stats.shape, stats.dtype)
    for d in range(side * side):
        labels[d] = 0
    for j in range(per_seq):
        for q in range(seqs):
            target = dest[j, q]
            labels[lax.div(target, held)] = lax.rem(target, held) * seqs + q + 1
    sorting = line_order(slots, owned, core == 1)
    first_load.wait()
    order[...] = jnp.dot(plain[...], sorting, preferred_element_type=F32).astype(BF16)

    sends = []
    row = lax.broadcasted_iota(jnp.int32, (PIECES, slots), 0)
    for q in range(seqs):
        arrivals[q].wait()
        feats = held_tokens[q]
        logits = jnp.dot(feats, order[...], preferred_element_type=F32)
        count = lengths[0, q] - shard * length
        live = lax.broadcasted_iota(jnp.int32, (length, 1), 0) < count
        masked = jnp.where(live, logits, NO_TOKEN)
        top = jnp.max(masked, axis=0, keepdims=True)
        weight = jnp.where(live, jnp.exp(masked - top), 0.0)
        mass = jnp.sum(weight, axis=0, keepdims=True)
        sums[q] = lax.dot_general(
            weight.astype(BF16), feats, (((0,), (0,)), ((), ())), preferred_element_type=F32
        ).astype(BF16)
        for k, part in enumerate(parts):
            first = pl.multiple_of(lax.rem(line + k, side) * group, group)
            numer = sums[q, pl.ds(first, group), :]
            for j in range(slabs):
                start = (j * seqs + q) * owned
                piece = numer[:, j * LANES : (j + 1) * LANES]
                part[:, start : start + owned, :] = piece.reshape(side, owned, LANES)
        stacked = jnp.zeros((PIECES, slots), F32)
        for k, piece in enumerate(pieces_of(top) + pieces_of(mass)):
            stacked = jnp.where(row == k, piece, stacked)
        stats[q * PIECES : (q + 1) * PIECES, :] = stacked

        peak = jnp.max(logits, axis=1, keepdims=True)
        raised = jnp.exp(logits - peak)
        mix = raised * (1.0 / jnp.sum(raised, axis=1, keepdims=True))
        blocks[q] = jnp.where(live, mix, 0.0).astype(BF16)
        for j in range(per_seq):
            target = mixes.at[lax.div(dest[j, q], held)]
            sends.append(
                pltpu.make_async_copy(
                    blocks.at[q, pl.ds(j * block, block)], target, sems.at[q, j]
                )
            )
            sends[-1].start()

    turned[...] = stats[...].T
    lane = lax.broadcasted_iota(jnp.int32, (owned, LANES), 1)
    for k, part in enumerate(parts):
        ahead = lax.rem(line + k, side)
        mine = turned[pl.ds(pl.multiple_of(ahead * group, group), group), :]
        for n in range(side):
            target = jnp.where(core == 1, n * side + ahead, ahead * side + n)
            tag = labels[target].astype(F32)
            piece = jnp.where(lane == TAGS + line, tag, mine[n * owned : (n + 1) * owned])
            part[n, stat_rows:, :] = piece.astype(BF16)
    for send in sends:
        send.wait()


def dispatch(tokens, params, lengths, dest, place, side):
    seqs, length, width = tokens.shape[1:]
    slots = params.shape[1]
    owned = slots // (side * side)
    rows = width // LANES * seqs * owned + owned
    per_seq = dest.shape[0]
    block = length // per_seq
    return pl.pallas_call(
        dispatch_kernel,
        in_specs=[SCALARS, SCALARS, SCALARS, ANYWHERE, ANYWHERE],
        out_specs=[WHOLE] * side + [ANYWHERE],
        scratch_shapes=[
            pltpu.VMEM((width, slots), BF16),
            pltpu.VMEM((width, slots), BF16),
            pltpu.VMEM((seqs, length, width), BF16),
            pltpu.VMEM((seqs, slots, width), BF16),
            pltpu.VMEM((slots, LANES), F32),
            pltpu.VMEM((LANES, slots), F32),
            pltpu.SMEM((side * side,), jnp.int32),
            pltpu.VMEM((seqs, length, slots), BF16),
            pltpu.SemaphoreType.DMA((seqs + 1,)),
            pltpu.SemaphoreType.DMA((seqs, per_seq)),
        ],
        out_shape=[pltpu.VMEM((side, rows, LANES), BF16)] * side
        + [pltpu.HBM((side * side, block, slots), BF16)],
        compiler_params=small(24),
        name="dispatch",
    )(*in_hbm(lengths, dest), place, *in_hbm(tokens, params))


def joined_stats(raws):
    tops = [raw + pltpu.roll(raw, LANES - 1, 1) + pltpu.roll(raw, LANES - 2, 1) for raw in raws]
    top = functools.reduce(jnp.maximum, tops)
    factors = [jnp.exp(each - top) for each in tops]
    mass = sum(each * pltpu.roll(factor, 3, 1) for each, factor in zip(tops, factors))
    return top, mass, factors


def merge_kernel(place, *refs):
    side = 4
    sources, results = refs[:side], refs[side:]
    rows = sources[0].shape[1]
    owned = 16
    seqs = 4
    stat_rows = rows - owned
    slabs = stat_rows // (seqs * owned)
    lane = lax.broadcasted_iota(jnp.int32, (owned, LANES), 1)
    for k, result in enumerate(results):
        ahead = lax.rem(place[3] + k, side)
        raws = [source[ahead, stat_rows:, :].astype(F32) for source in sources]
        top, mass, factors = joined_stats(raws)
        stat = jnp.where(lane >= TAGS, sum(raws), 0.0)
        for value, first in ((top, 0), (mass, 3)):
            for n, piece in enumerate(pieces_of(value)):
                spread = pltpu.roll(piece, n, 1) if n else piece
                stat = jnp.where((lane < TAGS) & (lane % PIECES == first + n), spread, stat)
        result[stat_rows:, :] = stat.astype(BF16)
        for q in range(seqs):
            columns = [factor[:, q * PIECES : q * PIECES + 1] for factor in factors]
            for j in range(slabs):
                start = (j * seqs + q) * owned
                total = sum(
                    source[ahead, start : start + owned, :].astype(F32) * column
                    for source, column in zip(sources, columns)
                )
                result[start : start + owned, :] = total.astype(BF16)


def merge(place, parts):
    side, rows, _ = parts[0].shape
    return pl.pallas_call(
        merge_kernel,
        in_specs=[SCALARS] + [WHOLE] * side,
        out_specs=[WHOLE] * side,
        out_shape=[pltpu.VMEM((rows, LANES), BF16)] * side,
        compiler_params=small(4),
        name="merge",
    )(place, *in_vmem(*parts))


def expert_order(seqs, experts, per_expert, back):
    total = seqs * experts * per_expert
    here = lax.broadcasted_iota(jnp.int32, (total, total), 1 if back else 0)
    there = lax.broadcasted_iota(jnp.int32, (total, total), 0 if back else 1)
    expert = here // (seqs * per_expert)
    seq = here // per_expert % seqs
    rank = here % per_expert
    return (there == (seq * experts + expert) * per_expert + rank).astype(BF16)


def own_kernel(seqs, experts, *refs):
    received, (result, labels) = refs[:-2], refs[-2:]
    rows, _ = received[0].shape
    owned = result.shape[0] // seqs
    stat_rows = rows - owned
    slabs = stat_rows // (seqs * owned)
    raws = [source[stat_rows:, :].astype(F32) for source in received]
    for k, raw in enumerate(raws):
        labels[k : k + 1, :] = raw[:1]
    _, mass, factors = joined_stats(raws)
    mass = pltpu.roll(mass, LANES - 3, 1)
    parts = []
    for q in range(seqs):
        totals = [jnp.zeros((owned, LANES), F32)] * slabs
        for source, factor in zip(received, factors):
            column = (factor / mass)[:, q * PIECES : q * PIECES + 1]
            for j in range(slabs):
                start = (j * seqs + q) * owned
                totals[j] += source[start : start + owned, :].astype(F32) * column
        parts.append(jnp.concatenate(totals, axis=1))
    slot_in = jnp.concatenate(parts, axis=0).astype(BF16)
    order = expert_order(seqs, experts, owned // experts, False)
    ordered = jnp.dot(order, slot_in, preferred_element_type=F32).astype(BF16)
    result[...] = ordered


def own_slots(received, seqs, experts, owned):
    rows, _ = received[0].shape
    width = (rows - owned) // (seqs * owned) * LANES
    return pl.pallas_call(
        functools.partial(own_kernel, seqs, experts),
        in_specs=[WHOLE] * len(received),
        out_specs=[WHOLE, WHOLE],
        out_shape=[
            pltpu.VMEM((seqs * owned, width), BF16),
            jax.ShapeDtypeStruct((len(received), LANES), F32),
        ],
        compiler_params=small(4),
        name="own_slots",
    )(*in_vmem(*received))


def gelu(x):
    return 0.5 * x * (1.0 + jnp.tanh(math.sqrt(2.0 / math.pi) * (x + 0.044715 * (x * x * x))))


def expert_kernel(count, *refs):
    rows = refs[:count]
    first_far, second_far, own_out, other_out, first, second, sems = refs[count:]
    experts = first.shape[0]
    each = rows[0].shape[0] // experts
    half = count // 2
    loads = []
    for e in range(experts):
        loads.append(pltpu.make_async_copy(first_far.at[e], first.at[e], sems.at[0, e]))
        loads.append(pltpu.make_async_copy(second_far.at[e], second.at[e], sems.at[1, e]))
    for load in loads:
        load.start()
    for e in range(experts):
        span = slice(e * each, (e + 1) * each)
        both = jnp.concatenate([ref[span, :] for ref in rows], axis=0)
        loads[2 * e].wait()
        hidden = gelu(jnp.dot(both, first[e], preferred_element_type=F32)).astype(BF16)
        loads[2 * e + 1].wait()
        result = jnp.dot(hidden, second[e], preferred_element_type=F32)
        for k in range(half):
            own_out[k, span, :] = result[k * each : (k + 1) * each]
            other = result[(half + k) * each : (half + k + 1) * each]
            other_out[k, span, :] = other.astype(BF16)


def expert_layers(own, other, first, second):
    shape = (len(own), *own[0].shape)
    count = len(own) + len(other)
    return pl.pallas_call(
        functools.partial(expert_kernel, count),
        in_specs=[WHOLE] * count + [ANYWHERE, ANYWHERE],
        out_specs=[WHOLE, WHOLE],
        out_shape=[pltpu.VMEM(shape, F32), pltpu.VMEM(shape, BF16)],
        scratch_shapes=[
            pltpu.VMEM(first.shape, first.dtype),
            pltpu.VMEM(second.shape, second.dtype),
            pltpu.SemaphoreType.DMA((2, first.shape[0])),
        ],
        compiler_params=small(24),
        name="experts",
    )(*in_vmem(*own, *other), *in_hbm(first, second))


def join_kernel(own, other, kept, *sent):
    kept[...] = own[0] + other[0].astype(F32)
    for k, ref in enumerate(sent):
        ref[...] = (own[k + 1] + other[k + 1].astype(F32)).astype(BF16)


def join(own, other):
    copies, rows, width = own.shape
    return pl.pallas_call(
        join_kernel,
        in_specs=[WHOLE, WHOLE],
        out_specs=[WHOLE] * copies,
        out_shape=[pltpu.VMEM((rows, width), F32)] + [pltpu.VMEM((rows, width), BF16)] * (copies - 1),
        compiler_params=small(4),
        name="join",
    )(*in_vmem(own, other))


def collect_kernel(seqs, experts, kept, *refs):
    result = refs[-1]
    total = kept[...]
    for ref in refs[:-1]:
        total += ref[...].astype(F32)
    total = total.astype(BF16)
    per_expert = total.shape[0] // (seqs * experts)
    order = expert_order(seqs, experts, per_expert, True)
    result[...] = jnp.dot(order, total, preferred_element_type=F32).astype(BF16)


def collect(kept, parts, seqs, experts):
    return pl.pallas_call(
        functools.partial(collect_kernel, seqs, experts),
        in_specs=[WHOLE] * (1 + len(parts)),
        out_specs=WHOLE,
        out_shape=pltpu.VMEM(kept.shape, BF16),
        compiler_params=small(4),
        name="collect",
    )(*in_vmem(kept, *parts))


def stack_kernel(place, *refs):
    result = refs[-1]
    side = result.shape[0]
    for k, ref in enumerate(refs[:-1]):
        result[lax.rem(place[2] + side - k, side)] = ref[...]


def stack(place, pieces):
    return pl.pallas_call(
        stack_kernel,
        in_specs=[SCALARS] + [WHOLE] * len(pieces),
        out_specs=WHOLE,
        out_shape=pltpu.VMEM((len(pieces), *pieces[0].shape), BF16),
        compiler_params=small(4),
        name="stack",
    )(place, *in_vmem(*pieces))


def combine_kernel(source, seq, place, mix, *refs):
    lines, (result, slots, buffer, sems) = refs[:-4], refs[-4:]
    side, rows, _ = lines[0].shape
    seqs = slots.shape[0]
    owned = rows // seqs
    for k, line in enumerate(lines):
        column = lax.rem(place[3] + side - k, side) * owned
        for f in range(side):
            start = pl.multiple_of(f * side * owned + column, owned)
            for q in range(seqs):
                slots[q, pl.ds(start, owned), :] = line[f, q * owned : (q + 1) * owned, :]
    copies = []
    for b in range(result.shape[1]):
        chosen = slots[seq[b]]
        buffer[b] = jnp.dot(mix[source[b]], chosen, preferred_element_type=F32).astype(BF16)
        copies.append(pltpu.make_async_copy(buffer.at[b], result.at[0, b], sems.at[b]))
        copies[-1].start()
    for copy in copies:
        copy.wait()


def combine(source, seq, place, mixes, lines, seqs):
    _, block, slots = mixes.shape
    width = lines[0].shape[2]
    blocks = source.shape[0]
    return pl.pallas_call(
        combine_kernel,
        in_specs=[SCALARS, SCALARS, SCALARS] + [WHOLE] * (1 + len(lines)),
        out_specs=ANYWHERE,
        out_shape=pltpu.HBM((1, blocks, block, width), BF16),
        scratch_shapes=[
            pltpu.VMEM((seqs, slots, width), BF16),
            pltpu.VMEM((blocks, block, width), BF16),
            pltpu.SemaphoreType.DMA((blocks,)),
        ],
        compiler_params=small(16),
        name="combine",
    )(source, seq, place, *in_vmem(mixes, *lines))


def swapped(array):
    return lax.ppermute(array, "c", [(0, 1), (1, 0)])


def exchanged(array, axis):
    return lax.all_to_all(array, axis, split_axis=0, concat_axis=0, tiled=True)


def moved(array, axis, step):
    size = lax.axis_size(axis)
    return lax.ppermute(array, axis, [(i, (i + step) % size) for i in range(size)])


def along(array, first, step):
    side = lax.axis_size("z")
    pairs = []
    for c in range(lax.axis_size("c")):
        for z in range(side):
            for x in range(side):
                in_z = first == (c == 0)
                to_z, to_x = ((z + step) % side, x) if in_z else (z, (x + step) % side)
                pairs.append(((c * side + z) * side + x, (c * side + to_z) * side + to_x))
    return lax.ppermute(array, ("c",) + EXPERT, pairs)


def local(tokens, slot_params, dest, lengths, w_in, w_out):
    seqs, _ = tokens.shape[1:3]
    held = dest.shape[1] * dest.shape[2]
    side = lax.axis_size("z")
    experts = w_in.shape[0]
    owned = slot_params.shape[1] // (side * side)
    planes = lax.axis_size("y")
    z, x, core = lax.axis_index("z"), lax.axis_index("x"), lax.axis_index("c")
    swap = core == 1
    place = jnp.stack([z * side + x, core, jnp.where(swap, x, z), jnp.where(swap, z, x)])
    table = dest[0].T

    *parts, mixes = dispatch(tokens, slot_params, lengths, table, place, side)
    steps = range(1, side)
    parts = merge(place, [parts[0]] + [along(parts[k], True, k) for k in steps])
    received = [parts[0]] + [along(parts[k], False, k) for k in steps]
    slot_in, tags = own_slots(received, seqs, experts, owned)
    mixes, slot_in = lax.optimization_barrier((mixes, slot_in))
    arrived = exchanged(mixes, EXPERT)
    own = [slot_in] + [moved(slot_in, "y", k) for k in range(1, planes)]

    other = [swapped(piece) for piece in own]
    own_out, other_out = expert_layers(own, other, w_in, w_out)
    kept, *sent = join(own_out, swapped(other_out))
    parts = [moved(piece, "y", -k - 1) for k, piece in enumerate(sent)]
    slot_out = collect(kept, parts, seqs, experts)

    found = tags[:, TAGS : TAGS + side].astype(jnp.int32) - 1
    line = jnp.arange(side, dtype=jnp.int32)[None, :]
    across = (place[3] - jnp.arange(side, dtype=jnp.int32)[:, None]) % side
    shard = jnp.where(swap, across * side + line, line * side + across).reshape(-1)
    found = found.reshape(-1)
    block = jnp.where(found >= 0, found // seqs, -1)
    match = block[None, :] == jnp.arange(held, dtype=jnp.int32)[:, None]
    source = jnp.sum(jnp.where(match, shard[None, :], 0), axis=1)
    seq = jnp.sum(jnp.where(match, found[None, :] % seqs, 0), axis=1)

    pieces = stack(place, [slot_out] + [along(slot_out, True, k) for k in steps])
    lines = [pieces] + [along(pieces, False, k) for k in steps]
    return combine(source, seq, place, arrived, lines, seqs)


def solution(mesh):
    finer = Mesh(mesh.devices.reshape(4, 2, 4, 4), DP + EXPERT)
    in_specs = (
        P(DP, None, EXPERT, None),
        P(),
        P(DP, None, EXPERT),
        P(DP, None),
        P(EXPERT, None, DP),
        P(EXPERT, DP, None),
    )
    out_specs = P(DP, EXPERT, None, None)
    return jax.shard_map(local, mesh=finer, in_specs=in_specs, out_specs=out_specs, check_vma=False)
```

```python
import functools
import math

import jax
import jax.numpy as jnp
from jax import lax
from jax.experimental import pallas as pl
from jax.experimental.pallas import tpu as pltpu
from jax.sharding import Mesh
from jax.sharding import PartitionSpec as P


DP = ("y", "c")
EXPERT = ("z", "x")
LANES = 128
PIECES = 8
TAGS = 64
NO_TOKEN = -1e30
F32 = jnp.float32
BF16 = jnp.bfloat16


def pieces_of(value):
    high = value.astype(BF16).astype(F32)
    rest = value - high
    middle = rest.astype(BF16).astype(F32)
    return high, middle, rest - middle


def small(mebibytes):
    return pltpu.CompilerParams(vmem_limit_bytes=mebibytes * 1024 * 1024)


def in_vmem(*arrays):
    return [pltpu.with_memory_space_constraint(array, pltpu.VMEM) for array in arrays]


def in_hbm(*arrays):
    return [pltpu.with_memory_space_constraint(array, pltpu.HBM) for array in arrays]


ANYWHERE = pl.BlockSpec(memory_space=pl.ANY)
WHOLE = pl.BlockSpec(memory_space=pltpu.VMEM)
SCALARS = pl.BlockSpec(memory_space=pltpu.SMEM)


def line_order(total, owned, swap):
    side = math.isqrt(total // owned)
    column = lax.broadcasted_iota(jnp.int32, (total, total), 1)
    place = column // owned
    shard = jnp.where(swap, place % side * side + place // side, place)
    source = shard * owned + column % owned
    return (lax.broadcasted_iota(jnp.int32, (total, total), 0) == source).astype(BF16)


def dispatch_kernel(lengths, dest, place, tokens, params, *refs):
    side = 4
    parts = refs[:side]
    plain, order, held_tokens, sums, turned, stats, labels, loads = refs[side:]
    shard, core, line = place[0], place[1], place[2]
    _, seqs, length, width = tokens.shape
    slots = params.shape[1]
    owned = slots // (side * side)
    slabs = width // LANES
    stat_rows = parts[0].shape[1] - owned
    per_seq = dest.shape[0]
    held = per_seq * seqs
    group = side * owned

    first_load = pltpu.make_async_copy(params, plain, loads.at[seqs])
    first_load.start()
    arrivals = []
    for q in range(seqs):
        arrivals.append(pltpu.make_async_copy(tokens.at[0, q], held_tokens.at[q], loads.at[q]))
        arrivals[-1].start()
    stats[...] = jnp.zeros(stats.shape, stats.dtype)
    for d in range(side * side):
        labels[d] = 0
    for j in range(per_seq):
        for q in range(seqs):
            target = dest[j, q]
            labels[lax.div(target, held)] = lax.rem(target, held) * seqs + q + 1
    sorting = line_order(slots, owned, core == 1)
    first_load.wait()
    order[...] = jnp.dot(plain[...], sorting, preferred_element_type=F32).astype(BF16)

    row = lax.broadcasted_iota(jnp.int32, (PIECES, slots), 0)
    for q in range(seqs):
        arrivals[q].wait()
        feats = held_tokens[q]
        logits = jnp.dot(feats, order[...], preferred_element_type=F32)
        count = lengths[0, q] - shard * length
        live = lax.broadcasted_iota(jnp.int32, (length, 1), 0) < count
        masked = jnp.where(live, logits, NO_TOKEN)
        top = jnp.max(masked, axis=0, keepdims=True)
        weight = jnp.where(live, jnp.exp(masked - top), 0.0)
        mass = jnp.sum(weight, axis=0, keepdims=True)
        sums[q] = lax.dot_general(
            weight.astype(BF16), feats, (((0,), (0,)), ((), ())), preferred_element_type=F32
        ).astype(BF16)
        for k, part in enumerate(parts):
            first = pl.multiple_of(lax.rem(line + k, side) * group, group)
            numer = sums[q, pl.ds(first, group), :]
            for j in range(slabs):
                start = (j * seqs + q) * owned
                piece = numer[:, j * LANES : (j + 1) * LANES]
                part[:, start : start + owned, :] = piece.reshape(side, owned, LANES)
        stacked = jnp.zeros((PIECES, slots), F32)
        for k, piece in enumerate(pieces_of(top) + pieces_of(mass)):
            stacked = jnp.where(row == k, piece, stacked)
        stats[q * PIECES : (q + 1) * PIECES, :] = stacked

    turned[...] = stats[...].T
    lane = lax.broadcasted_iota(jnp.int32, (owned, LANES), 1)
    for k, part in enumerate(parts):
        ahead = lax.rem(line + k, side)
        mine = turned[pl.ds(pl.multiple_of(ahead * group, group), group), :]
        for n in range(side):
            target = jnp.where(core == 1, n * side + ahead, ahead * side + n)
            tag = labels[target].astype(F32)
            piece = jnp.where(lane == TAGS + line, tag, mine[n * owned : (n + 1) * owned])
            part[n, stat_rows:, :] = piece.astype(BF16)


def mix_kernel(lengths, dest, place, tokens, params, mixes, plain, held_tokens, blocks, loads, sems):
    shard, core = place[0], place[1]
    _, seqs, length, _ = tokens.shape
    slots = params.shape[1]
    block = mixes.shape[1]
    per_seq = length // block
    held = per_seq * seqs
    first_load = pltpu.make_async_copy(params, plain, loads.at[seqs])
    first_load.start()
    arrivals = []
    for q in range(seqs):
        arrivals.append(pltpu.make_async_copy(tokens.at[0, q], held_tokens.at[q], loads.at[q]))
        arrivals[-1].start()
    sorting = line_order(slots, slots // mixes.shape[0], core == 1)
    first_load.wait()
    order = jnp.dot(plain[...], sorting, preferred_element_type=F32).astype(BF16)
    sends = []
    for q in range(seqs):
        arrivals[q].wait()
        logits = jnp.dot(held_tokens[q], order, preferred_element_type=F32)
        count = lengths[0, q] - shard * length
        live = lax.broadcasted_iota(jnp.int32, (length, 1), 0) < count
        peak = jnp.max(logits, axis=1, keepdims=True)
        raised = jnp.exp(logits - peak)
        mix = raised * (1.0 / jnp.sum(raised, axis=1, keepdims=True))
        blocks[q] = jnp.where(live, mix, 0.0).astype(BF16)
        for j in range(per_seq):
            target = mixes.at[lax.div(dest[j, q], held)]
            sends.append(
                pltpu.make_async_copy(
                    blocks.at[q, pl.ds(j * block, block)], target, sems.at[q, j]
                )
            )
            sends[-1].start()
    for send in sends:
        send.wait()


def mix_rows(tokens, params, lengths, dest, place, side):
    _, seqs, length, width = tokens.shape
    slots = params.shape[1]
    per_seq = dest.shape[0]
    return pl.pallas_call(
        mix_kernel,
        in_specs=[SCALARS, SCALARS, SCALARS, ANYWHERE, ANYWHERE],
        out_specs=ANYWHERE,
        scratch_shapes=[
            pltpu.VMEM((width, slots), BF16),
            pltpu.VMEM((seqs, length, width), BF16),
            pltpu.VMEM((seqs, length, slots), BF16),
            pltpu.SemaphoreType.DMA((seqs + 1,)),
            pltpu.SemaphoreType.DMA((seqs, per_seq)),
        ],
        out_shape=pltpu.HBM((side * side, length // per_seq, slots), BF16),
        compiler_params=small(16),
        name="mix_rows",
    )(*in_hbm(lengths, dest), place, *in_hbm(tokens, params))


def dispatch(tokens, params, lengths, dest, place, side):
    seqs, length, width = tokens.shape[1:]
    slots = params.shape[1]
    owned = slots // (side * side)
    rows = width // LANES * seqs * owned + owned
    return pl.pallas_call(
        dispatch_kernel,
        in_specs=[SCALARS, SCALARS, SCALARS, ANYWHERE, ANYWHERE],
        out_specs=[WHOLE] * side,
        scratch_shapes=[
            pltpu.VMEM((width, slots), BF16),
            pltpu.VMEM((width, slots), BF16),
            pltpu.VMEM((seqs, length, width), BF16),
            pltpu.VMEM((seqs, slots, width), BF16),
            pltpu.VMEM((slots, LANES), F32),
            pltpu.VMEM((LANES, slots), F32),
            pltpu.SMEM((side * side,), jnp.int32),
            pltpu.SemaphoreType.DMA((seqs + 1,)),
        ],
        out_shape=[pltpu.VMEM((side, rows, LANES), BF16)] * side,
        compiler_params=small(24),
        name="dispatch",
    )(*in_hbm(lengths, dest), place, *in_hbm(tokens, params))


def joined_stats(raws):
    tops = [raw + pltpu.roll(raw, LANES - 1, 1) + pltpu.roll(raw, LANES - 2, 1) for raw in raws]
    top = functools.reduce(jnp.maximum, tops)
    factors = [jnp.exp(each - top) for each in tops]
    mass = sum(each * pltpu.roll(factor, 3, 1) for each, factor in zip(tops, factors))
    return top, mass, factors


def merge_kernel(place, *refs):
    side = 4
    sources, results = refs[:side], refs[side:]
    rows = sources[0].shape[1]
    owned = 16
    seqs = 4
    stat_rows = rows - owned
    slabs = stat_rows // (seqs * owned)
    lane = lax.broadcasted_iota(jnp.int32, (owned, LANES), 1)
    for k, result in enumerate(results):
        ahead = lax.rem(place[3] + k, side)
        raws = [source[ahead, stat_rows:, :].astype(F32) for source in sources]
        top, mass, factors = joined_stats(raws)
        stat = jnp.where(lane >= TAGS, sum(raws), 0.0)
        for value, first in ((top, 0), (mass, 3)):
            for n, piece in enumerate(pieces_of(value)):
                spread = pltpu.roll(piece, n, 1) if n else piece
                stat = jnp.where((lane < TAGS) & (lane % PIECES == first + n), spread, stat)
        result[stat_rows:, :] = stat.astype(BF16)
        for q in range(seqs):
            columns = [factor[:, q * PIECES : q * PIECES + 1] for factor in factors]
            for j in range(slabs):
                start = (j * seqs + q) * owned
                total = sum(
                    source[ahead, start : start + owned, :].astype(F32) * column
                    for source, column in zip(sources, columns)
                )
                result[start : start + owned, :] = total.astype(BF16)


def merge(place, parts):
    side, rows, _ = parts[0].shape
    return pl.pallas_call(
        merge_kernel,
        in_specs=[SCALARS] + [WHOLE] * side,
        out_specs=[WHOLE] * side,
        out_shape=[pltpu.VMEM((rows, LANES), BF16)] * side,
        compiler_params=small(4),
        name="merge",
    )(place, *in_vmem(*parts))


def expert_order(seqs, experts, per_expert, back):
    total = seqs * experts * per_expert
    here = lax.broadcasted_iota(jnp.int32, (total, total), 1 if back else 0)
    there = lax.broadcasted_iota(jnp.int32, (total, total), 0 if back else 1)
    expert = here // (seqs * per_expert)
    seq = here // per_expert % seqs
    rank = here % per_expert
    return (there == (seq * experts + expert) * per_expert + rank).astype(BF16)


def own_kernel(seqs, experts, *refs):
    received, (result, labels) = refs[:-2], refs[-2:]
    rows, _ = received[0].shape
    owned = result.shape[0] // seqs
    stat_rows = rows - owned
    slabs = stat_rows // (seqs * owned)
    raws = [source[stat_rows:, :].astype(F32) for source in received]
    for k, raw in enumerate(raws):
        labels[k : k + 1, :] = raw[:1]
    _, mass, factors = joined_stats(raws)
    mass = pltpu.roll(mass, LANES - 3, 1)
    parts = []
    for q in range(seqs):
        totals = [jnp.zeros((owned, LANES), F32)] * slabs
        for source, factor in zip(received, factors):
            column = (factor / mass)[:, q * PIECES : q * PIECES + 1]
            for j in range(slabs):
                start = (j * seqs + q) * owned
                totals[j] += source[start : start + owned, :].astype(F32) * column
        parts.append(jnp.concatenate(totals, axis=1))
    slot_in = jnp.concatenate(parts, axis=0).astype(BF16)
    order = expert_order(seqs, experts, owned // experts, False)
    ordered = jnp.dot(order, slot_in, preferred_element_type=F32).astype(BF16)
    result[...] = ordered


def own_slots(received, seqs, experts, owned):
    rows, _ = received[0].shape
    width = (rows - owned) // (seqs * owned) * LANES
    return pl.pallas_call(
        functools.partial(own_kernel, seqs, experts),
        in_specs=[WHOLE] * len(received),
        out_specs=[WHOLE, WHOLE],
        out_shape=[
            pltpu.VMEM((seqs * owned, width), BF16),
            jax.ShapeDtypeStruct((len(received), LANES), F32),
        ],
        compiler_params=small(4),
        name="own_slots",
    )(*in_vmem(*received))


def gelu(x):
    return 0.5 * x * (1.0 + jnp.tanh(math.sqrt(2.0 / math.pi) * (x + 0.044715 * (x * x * x))))


def fetch_kernel(first, second, first_out, second_out, sems):
    copies = []
    for e in range(first.shape[0]):
        copies.append(pltpu.make_async_copy(first.at[e], first_out.at[e], sems.at[0, e]))
        copies.append(pltpu.make_async_copy(second.at[e], second_out.at[e], sems.at[1, e]))
    for copy in copies:
        copy.start()
    for copy in copies:
        copy.wait()


def fetch(first, second):
    return pl.pallas_call(
        fetch_kernel,
        in_specs=[ANYWHERE, ANYWHERE],
        out_specs=[WHOLE, WHOLE],
        out_shape=[pltpu.VMEM(first.shape, first.dtype), pltpu.VMEM(second.shape, second.dtype)],
        scratch_shapes=[pltpu.SemaphoreType.DMA((2, first.shape[0]))],
        compiler_params=small(1),
        name="fetch",
    )(*in_hbm(first, second))


def expert_kernel(count, *refs):
    rows = refs[:count]
    first, second, own_out, other_out = refs[count:]
    experts = first.shape[0]
    each = rows[0].shape[0] // experts
    half = count // 2
    for e in range(experts):
        span = slice(e * each, (e + 1) * each)
        both = jnp.concatenate([ref[span, :] for ref in rows], axis=0)
        hidden = gelu(jnp.dot(both, first[e], preferred_element_type=F32)).astype(BF16)
        result = jnp.dot(hidden, second[e], preferred_element_type=F32)
        for k in range(half):
            own_out[k, span, :] = result[k * each : (k + 1) * each]
            other = result[(half + k) * each : (half + k + 1) * each]
            other_out[k, span, :] = other.astype(BF16)


def expert_layers(own, other, first, second):
    shape = (len(own), *own[0].shape)
    count = len(own) + len(other)
    return pl.pallas_call(
        functools.partial(expert_kernel, count),
        in_specs=[WHOLE] * (count + 2),
        out_specs=[WHOLE, WHOLE],
        out_shape=[pltpu.VMEM(shape, F32), pltpu.VMEM(shape, BF16)],
        compiler_params=small(8),
        name="experts",
    )(*in_vmem(*own, *other, first, second))


def join_kernel(own, other, kept, *sent):
    kept[...] = own[0] + other[0].astype(F32)
    for k, ref in enumerate(sent):
        ref[...] = (own[k + 1] + other[k + 1].astype(F32)).astype(BF16)


def join(own, other):
    copies, rows, width = own.shape
    return pl.pallas_call(
        join_kernel,
        in_specs=[WHOLE, WHOLE],
        out_specs=[WHOLE] * copies,
        out_shape=[pltpu.VMEM((rows, width), F32)] + [pltpu.VMEM((rows, width), BF16)] * (copies - 1),
        compiler_params=small(4),
        name="join",
    )(*in_vmem(own, other))


def collect_kernel(seqs, experts, kept, *refs):
    result = refs[-1]
    total = kept[...]
    for ref in refs[:-1]:
        total += ref[...].astype(F32)
    total = total.astype(BF16)
    per_expert = total.shape[0] // (seqs * experts)
    order = expert_order(seqs, experts, per_expert, True)
    result[...] = jnp.dot(order, total, preferred_element_type=F32).astype(BF16)


def collect(kept, parts, seqs, experts):
    return pl.pallas_call(
        functools.partial(collect_kernel, seqs, experts),
        in_specs=[WHOLE] * (1 + len(parts)),
        out_specs=WHOLE,
        out_shape=pltpu.VMEM(kept.shape, BF16),
        compiler_params=small(4),
        name="collect",
    )(*in_vmem(kept, *parts))


def stack_kernel(place, *refs):
    result = refs[-1]
    side = result.shape[0]
    for k, ref in enumerate(refs[:-1]):
        result[lax.rem(place[2] + side - k, side)] = ref[...]


def stack(place, pieces):
    return pl.pallas_call(
        stack_kernel,
        in_specs=[SCALARS] + [WHOLE] * len(pieces),
        out_specs=WHOLE,
        out_shape=pltpu.VMEM((len(pieces), *pieces[0].shape), BF16),
        compiler_params=small(4),
        name="stack",
    )(place, *in_vmem(*pieces))


def combine_kernel(source, seq, place, mix, *refs):
    lines, (result, slots, buffer, sems) = refs[:-4], refs[-4:]
    side, rows, _ = lines[0].shape
    seqs = slots.shape[0]
    owned = rows // seqs
    for k, line in enumerate(lines):
        column = lax.rem(place[3] + side - k, side) * owned
        for f in range(side):
            start = pl.multiple_of(f * side * owned + column, owned)
            for q in range(seqs):
                slots[q, pl.ds(start, owned), :] = line[f, q * owned : (q + 1) * owned, :]
    copies = []
    for b in range(result.shape[1]):
        chosen = slots[seq[b]]
        buffer[b] = jnp.dot(mix[source[b]], chosen, preferred_element_type=F32).astype(BF16)
        copies.append(pltpu.make_async_copy(buffer.at[b], result.at[0, b], sems.at[b]))
        copies[-1].start()
    for copy in copies:
        copy.wait()


def combine(source, seq, place, mixes, lines, seqs):
    _, block, slots = mixes.shape
    width = lines[0].shape[2]
    blocks = source.shape[0]
    return pl.pallas_call(
        combine_kernel,
        in_specs=[SCALARS, SCALARS, SCALARS] + [WHOLE] * (1 + len(lines)),
        out_specs=ANYWHERE,
        out_shape=pltpu.HBM((1, blocks, block, width), BF16),
        scratch_shapes=[
            pltpu.VMEM((seqs, slots, width), BF16),
            pltpu.VMEM((blocks, block, width), BF16),
            pltpu.SemaphoreType.DMA((blocks,)),
        ],
        compiler_params=small(16),
        name="combine",
    )(source, seq, place, *in_vmem(mixes, *lines))


def swapped(array):
    return lax.ppermute(array, "c", [(0, 1), (1, 0)])


def exchanged(array, axis):
    return lax.all_to_all(array, axis, split_axis=0, concat_axis=0, tiled=True)


def moved(array, axis, step):
    size = lax.axis_size(axis)
    return lax.ppermute(array, axis, [(i, (i + step) % size) for i in range(size)])


def along(array, first, step):
    side = lax.axis_size("z")
    pairs = []
    for c in range(lax.axis_size("c")):
        for z in range(side):
            for x in range(side):
                in_z = first == (c == 0)
                to_z, to_x = ((z + step) % side, x) if in_z else (z, (x + step) % side)
                pairs.append(((c * side + z) * side + x, (c * side + to_z) * side + to_x))
    return lax.ppermute(array, ("c",) + EXPERT, pairs)


def local(tokens, slot_params, dest, lengths, w_in, w_out):
    seqs, _ = tokens.shape[1:3]
    held = dest.shape[1] * dest.shape[2]
    side = lax.axis_size("z")
    experts = w_in.shape[0]
    owned = slot_params.shape[1] // (side * side)
    planes = lax.axis_size("y")
    z, x, core = lax.axis_index("z"), lax.axis_index("x"), lax.axis_index("c")
    swap = core == 1
    place = jnp.stack([z * side + x, core, jnp.where(swap, x, z), jnp.where(swap, z, x)])
    table = dest[0].T

    steps = range(1, side)
    parts = dispatch(tokens, slot_params, lengths, table, place, side)
    mixes = mix_rows(tokens, slot_params, lengths, table, place, side)
    parts = [parts[0]] + [along(parts[k], True, k) for k in steps]
    parts = merge(place, parts)
    mixes, *parts = lax.optimization_barrier((mixes, *parts))
    received = [parts[0]] + [along(parts[k], False, k) for k in steps]
    arrived = exchanged(mixes, EXPERT)
    slot_in, tags = own_slots(received, seqs, experts, owned)
    weights = fetch(w_in, w_out)
    own = [slot_in] + [moved(slot_in, "y", k) for k in range(1, planes)]

    other = [swapped(piece) for piece in own]
    own_out, other_out = expert_layers(own, other, *weights)
    kept, *sent = join(own_out, swapped(other_out))
    parts = [moved(piece, "y", -k - 1) for k, piece in enumerate(sent)]
    slot_out = collect(kept, parts, seqs, experts)

    found = tags[:, TAGS : TAGS + side].astype(jnp.int32) - 1
    line = jnp.arange(side, dtype=jnp.int32)[None, :]
    across = (place[3] - jnp.arange(side, dtype=jnp.int32)[:, None]) % side
    shard = jnp.where(swap, across * side + line, line * side + across).reshape(-1)
    found = found.reshape(-1)
    block = jnp.where(found >= 0, found // seqs, -1)
    match = block[None, :] == jnp.arange(held, dtype=jnp.int32)[:, None]
    source = jnp.sum(jnp.where(match, shard[None, :], 0), axis=1)
    seq = jnp.sum(jnp.where(match, found[None, :] % seqs, 0), axis=1)

    pieces = stack(place, [slot_out] + [along(slot_out, True, k) for k in steps])
    lines = [pieces] + [along(pieces, False, k) for k in steps]
    return combine(source, seq, place, arrived, lines, seqs)


def solution(mesh):
    finer = Mesh(mesh.devices.reshape(4, 2, 4, 4), DP + EXPERT)
    in_specs = (
        P(DP, None, EXPERT, None),
        P(),
        P(DP, None, EXPERT),
        P(DP, None),
        P(EXPERT, None, DP),
        P(EXPERT, DP, None),
    )
    out_specs = P(DP, EXPERT, None, None)
    return jax.shard_map(local, mesh=finer, in_specs=in_specs, out_specs=out_specs, check_vma=False)
```

```python
import functools
import math

import jax
import jax.numpy as jnp
from jax import lax
from jax.experimental import pallas as pl
from jax.experimental.pallas import tpu as pltpu
from jax.sharding import Mesh
from jax.sharding import PartitionSpec as P


DP = ("y", "c")
EXPERT = ("z", "x")
LANES = 128
PIECES = 8
TAGS = 64
NO_TOKEN = -1e30
F32 = jnp.float32
BF16 = jnp.bfloat16


def pieces_of(value):
    high = value.astype(BF16).astype(F32)
    rest = value - high
    middle = rest.astype(BF16).astype(F32)
    return high, middle, rest - middle


def small(mebibytes):
    return pltpu.CompilerParams(vmem_limit_bytes=mebibytes * 1024 * 1024)


def in_vmem(*arrays):
    return [pltpu.with_memory_space_constraint(array, pltpu.VMEM) for array in arrays]


def in_hbm(*arrays):
    return [pltpu.with_memory_space_constraint(array, pltpu.HBM) for array in arrays]


ANYWHERE = pl.BlockSpec(memory_space=pl.ANY)
WHOLE = pl.BlockSpec(memory_space=pltpu.VMEM)
SCALARS = pl.BlockSpec(memory_space=pltpu.SMEM)


def line_order(total, owned, swap):
    side = math.isqrt(total // owned)
    column = lax.broadcasted_iota(jnp.int32, (total, total), 1)
    place = column // owned
    shard = jnp.where(swap, place % side * side + place // side, place)
    source = shard * owned + column % owned
    return (lax.broadcasted_iota(jnp.int32, (total, total), 0) == source).astype(BF16)


def dispatch_kernel(lengths, dest, place, tokens, params, *refs):
    side = 4
    parts = refs[:side]
    plain, order, held_tokens, sums, turned, stats, labels, loads = refs[side:]
    shard, core, line = place[0], place[1], place[2]
    _, seqs, length, width = tokens.shape
    slots = params.shape[1]
    owned = slots // (side * side)
    slabs = width // LANES
    stat_rows = parts[0].shape[1] - owned
    per_seq = dest.shape[0]
    held = per_seq * seqs
    group = side * owned

    first_load = pltpu.make_async_copy(params, plain, loads.at[seqs])
    first_load.start()
    arrivals = []
    for q in range(seqs):
        arrivals.append(pltpu.make_async_copy(tokens.at[0, q], held_tokens.at[q], loads.at[q]))
        arrivals[-1].start()
    stats[...] = jnp.zeros(stats.shape, stats.dtype)
    for d in range(side * side):
        labels[d] = 0
    for j in range(per_seq):
        for q in range(seqs):
            target = dest[j, q]
            labels[lax.div(target, held)] = lax.rem(target, held) * seqs + q + 1
    sorting = line_order(slots, owned, core == 1)
    first_load.wait()
    order[...] = jnp.dot(plain[...], sorting, preferred_element_type=F32).astype(BF16)

    row = lax.broadcasted_iota(jnp.int32, (PIECES, slots), 0)
    for q in range(seqs):
        arrivals[q].wait()
        feats = held_tokens[q]
        logits = jnp.dot(feats, order[...], preferred_element_type=F32)
        count = lengths[0, q] - shard * length
        live = lax.broadcasted_iota(jnp.int32, (length, 1), 0) < count
        masked = jnp.where(live, logits, NO_TOKEN)
        top = jnp.max(masked, axis=0, keepdims=True)
        weight = jnp.where(live, jnp.exp(masked - top), 0.0)
        mass = jnp.sum(weight, axis=0, keepdims=True)
        sums[q] = lax.dot_general(
            weight.astype(BF16), feats, (((0,), (0,)), ((), ())), preferred_element_type=F32
        ).astype(BF16)
        for k, part in enumerate(parts):
            first = pl.multiple_of(lax.rem(line + k, side) * group, group)
            numer = sums[q, pl.ds(first, group), :]
            for j in range(slabs):
                start = (j * seqs + q) * owned
                piece = numer[:, j * LANES : (j + 1) * LANES]
                part[:, start : start + owned, :] = piece.reshape(side, owned, LANES)
        stacked = jnp.zeros((PIECES, slots), F32)
        for k, piece in enumerate(pieces_of(top) + pieces_of(mass)):
            stacked = jnp.where(row == k, piece, stacked)
        stats[q * PIECES : (q + 1) * PIECES, :] = stacked

    turned[...] = stats[...].T
    lane = lax.broadcasted_iota(jnp.int32, (owned, LANES), 1)
    for k, part in enumerate(parts):
        ahead = lax.rem(line + k, side)
        mine = turned[pl.ds(pl.multiple_of(ahead * group, group), group), :]
        for n in range(side):
            target = jnp.where(core == 1, n * side + ahead, ahead * side + n)
            tag = labels[target].astype(F32)
            piece = jnp.where(lane == TAGS + line, tag, mine[n * owned : (n + 1) * owned])
            part[n, stat_rows:, :] = piece.astype(BF16)


def mix_kernel(lengths, dest, place, tokens, params, mixes, plain, held_tokens, blocks, loads, sems):
    shard, core = place[0], place[1]
    _, seqs, length, _ = tokens.shape
    slots = params.shape[1]
    block = mixes.shape[1]
    per_seq = length // block
    held = per_seq * seqs
    first_load = pltpu.make_async_copy(params, plain, loads.at[seqs])
    first_load.start()
    arrivals = []
    for q in range(seqs):
        arrivals.append(pltpu.make_async_copy(tokens.at[0, q], held_tokens.at[q], loads.at[q]))
        arrivals[-1].start()
    sorting = line_order(slots, slots // mixes.shape[0], core == 1)
    first_load.wait()
    order = jnp.dot(plain[...], sorting, preferred_element_type=F32).astype(BF16)
    sends = []
    for q in range(seqs):
        arrivals[q].wait()
        logits = jnp.dot(held_tokens[q], order, preferred_element_type=F32)
        count = lengths[0, q] - shard * length
        live = lax.broadcasted_iota(jnp.int32, (length, 1), 0) < count
        peak = jnp.max(logits, axis=1, keepdims=True)
        raised = jnp.exp(logits - peak)
        mix = raised * (1.0 / jnp.sum(raised, axis=1, keepdims=True))
        blocks[q] = jnp.where(live, mix, 0.0).astype(BF16)
        for j in range(per_seq):
            target = mixes.at[lax.div(dest[j, q], held)]
            sends.append(
                pltpu.make_async_copy(
                    blocks.at[q, pl.ds(j * block, block)], target, sems.at[q, j]
                )
            )
            sends[-1].start()
    for send in sends:
        send.wait()


def mix_rows(tokens, params, lengths, dest, place, side):
    _, seqs, length, width = tokens.shape
    slots = params.shape[1]
    per_seq = dest.shape[0]
    return pl.pallas_call(
        mix_kernel,
        in_specs=[SCALARS, SCALARS, SCALARS, ANYWHERE, ANYWHERE],
        out_specs=ANYWHERE,
        scratch_shapes=[
            pltpu.VMEM((width, slots), BF16),
            pltpu.VMEM((seqs, length, width), BF16),
            pltpu.VMEM((seqs, length, slots), BF16),
            pltpu.SemaphoreType.DMA((seqs + 1,)),
            pltpu.SemaphoreType.DMA((seqs, per_seq)),
        ],
        out_shape=pltpu.HBM((side * side, length // per_seq, slots), BF16),
        compiler_params=small(16),
        name="mix_rows",
    )(*in_hbm(lengths, dest), place, *in_hbm(tokens, params))


def dispatch(tokens, params, lengths, dest, place, side):
    seqs, length, width = tokens.shape[1:]
    slots = params.shape[1]
    owned = slots // (side * side)
    rows = width // LANES * seqs * owned + owned
    return pl.pallas_call(
        dispatch_kernel,
        in_specs=[SCALARS, SCALARS, SCALARS, ANYWHERE, ANYWHERE],
        out_specs=[WHOLE] * side,
        scratch_shapes=[
            pltpu.VMEM((width, slots), BF16),
            pltpu.VMEM((width, slots), BF16),
            pltpu.VMEM((seqs, length, width), BF16),
            pltpu.VMEM((seqs, slots, width), BF16),
            pltpu.VMEM((slots, LANES), F32),
            pltpu.VMEM((LANES, slots), F32),
            pltpu.SMEM((side * side,), jnp.int32),
            pltpu.SemaphoreType.DMA((seqs + 1,)),
        ],
        out_shape=[pltpu.VMEM((side, rows, LANES), BF16)] * side,
        compiler_params=small(24),
        name="dispatch",
    )(*in_hbm(lengths, dest), place, *in_hbm(tokens, params))


def joined_stats(raws):
    tops = [raw + pltpu.roll(raw, LANES - 1, 1) + pltpu.roll(raw, LANES - 2, 1) for raw in raws]
    top = functools.reduce(jnp.maximum, tops)
    factors = [jnp.exp(each - top) for each in tops]
    mass = sum(each * pltpu.roll(factor, 3, 1) for each, factor in zip(tops, factors))
    return top, mass, factors


def merge_kernel(step, place, *refs):
    side = 4
    sources, results = refs[:side], refs[side:]
    rows = sources[0].shape[1]
    owned = 16
    seqs = 4
    stat_rows = rows - owned
    slabs = stat_rows // (seqs * owned)
    lane = lax.broadcasted_iota(jnp.int32, (owned, LANES), 1)
    for result in results:
        ahead = lax.rem(place[3] + step, side)
        raws = [source[ahead, stat_rows:, :].astype(F32) for source in sources]
        top, mass, factors = joined_stats(raws)
        stat = jnp.where(lane >= TAGS, sum(raws), 0.0)
        for value, first in ((top, 0), (mass, 3)):
            for n, piece in enumerate(pieces_of(value)):
                spread = pltpu.roll(piece, n, 1) if n else piece
                stat = jnp.where((lane < TAGS) & (lane % PIECES == first + n), spread, stat)
        result[stat_rows:, :] = stat.astype(BF16)
        for q in range(seqs):
            columns = [factor[:, q * PIECES : q * PIECES + 1] for factor in factors]
            for j in range(slabs):
                start = (j * seqs + q) * owned
                total = sum(
                    source[ahead, start : start + owned, :].astype(F32) * column
                    for source, column in zip(sources, columns)
                )
                result[start : start + owned, :] = total.astype(BF16)


def merge(place, parts, step):
    side, rows, _ = parts[0].shape
    return pl.pallas_call(
        functools.partial(merge_kernel, step),
        in_specs=[SCALARS] + [WHOLE] * side,
        out_specs=[WHOLE],
        out_shape=[pltpu.VMEM((rows, LANES), BF16)],
        compiler_params=small(4),
    )(place, *in_vmem(*parts))[0]


def expert_order(seqs, experts, per_expert, back):
    total = seqs * experts * per_expert
    here = lax.broadcasted_iota(jnp.int32, (total, total), 1 if back else 0)
    there = lax.broadcasted_iota(jnp.int32, (total, total), 0 if back else 1)
    expert = here // (seqs * per_expert)
    seq = here // per_expert % seqs
    rank = here % per_expert
    return (there == (seq * experts + expert) * per_expert + rank).astype(BF16)


def own_kernel(seqs, experts, *refs):
    received, (result, labels) = refs[:-2], refs[-2:]
    rows, _ = received[0].shape
    owned = result.shape[0] // seqs
    stat_rows = rows - owned
    slabs = stat_rows // (seqs * owned)
    raws = [source[stat_rows:, :].astype(F32) for source in received]
    for k, raw in enumerate(raws):
        labels[k : k + 1, :] = raw[:1]
    _, mass, factors = joined_stats(raws)
    mass = pltpu.roll(mass, LANES - 3, 1)
    parts = []
    for q in range(seqs):
        totals = [jnp.zeros((owned, LANES), F32)] * slabs
        for source, factor in zip(received, factors):
            column = (factor / mass)[:, q * PIECES : q * PIECES + 1]
            for j in range(slabs):
                start = (j * seqs + q) * owned
                totals[j] += source[start : start + owned, :].astype(F32) * column
        parts.append(jnp.concatenate(totals, axis=1))
    slot_in = jnp.concatenate(parts, axis=0).astype(BF16)
    order = expert_order(seqs, experts, owned // experts, False)
    ordered = jnp.dot(order, slot_in, preferred_element_type=F32).astype(BF16)
    result[...] = ordered


def own_slots(received, seqs, experts, owned):
    rows, _ = received[0].shape
    width = (rows - owned) // (seqs * owned) * LANES
    return pl.pallas_call(
        functools.partial(own_kernel, seqs, experts),
        in_specs=[WHOLE] * len(received),
        out_specs=[WHOLE, WHOLE],
        out_shape=[
            pltpu.VMEM((seqs * owned, width), BF16),
            jax.ShapeDtypeStruct((len(received), LANES), F32),
        ],
        compiler_params=small(4),
        name="own_slots",
    )(*in_vmem(*received))


def gelu(x):
    return 0.5 * x * (1.0 + jnp.tanh(math.sqrt(2.0 / math.pi) * (x + 0.044715 * (x * x * x))))


def fetch_kernel(first, second, first_out, second_out, sems):
    copies = []
    for e in range(first.shape[0]):
        copies.append(pltpu.make_async_copy(first.at[e], first_out.at[e], sems.at[0, e]))
        copies.append(pltpu.make_async_copy(second.at[e], second_out.at[e], sems.at[1, e]))
    for copy in copies:
        copy.start()
    for copy in copies:
        copy.wait()


def fetch(first, second):
    return pl.pallas_call(
        fetch_kernel,
        in_specs=[ANYWHERE, ANYWHERE],
        out_specs=[WHOLE, WHOLE],
        out_shape=[pltpu.VMEM(first.shape, first.dtype), pltpu.VMEM(second.shape, second.dtype)],
        scratch_shapes=[pltpu.SemaphoreType.DMA((2, first.shape[0]))],
        compiler_params=small(1),
        name="fetch",
    )(*in_hbm(first, second))


def expert_kernel(count, *refs):
    rows = refs[:count]
    first, second, own_out, other_out = refs[count:]
    experts = first.shape[0]
    each = rows[0].shape[0] // experts
    half = count // 2
    for e in range(experts):
        span = slice(e * each, (e + 1) * each)
        both = jnp.concatenate([ref[span, :] for ref in rows], axis=0)
        hidden = gelu(jnp.dot(both, first[e], preferred_element_type=F32)).astype(BF16)
        result = jnp.dot(hidden, second[e], preferred_element_type=F32)
        for k in range(half):
            own_out[k, span, :] = result[k * each : (k + 1) * each]
            other = result[(half + k) * each : (half + k + 1) * each]
            other_out[k, span, :] = other.astype(BF16)


def expert_layers(own, other, first, second):
    shape = (len(own), *own[0].shape)
    count = len(own) + len(other)
    return pl.pallas_call(
        functools.partial(expert_kernel, count),
        in_specs=[WHOLE] * (count + 2),
        out_specs=[WHOLE, WHOLE],
        out_shape=[pltpu.VMEM(shape, F32), pltpu.VMEM(shape, BF16)],
        compiler_params=small(8),
        name="experts",
    )(*in_vmem(*own, *other, first, second))


def join_kernel(own, other, kept, *sent):
    kept[...] = own[0] + other[0].astype(F32)
    for k, ref in enumerate(sent):
        ref[...] = (own[k + 1] + other[k + 1].astype(F32)).astype(BF16)


def join(own, other):
    copies, rows, width = own.shape
    return pl.pallas_call(
        join_kernel,
        in_specs=[WHOLE, WHOLE],
        out_specs=[WHOLE] * copies,
        out_shape=[pltpu.VMEM((rows, width), F32)] + [pltpu.VMEM((rows, width), BF16)] * (copies - 1),
        compiler_params=small(4),
        name="join",
    )(*in_vmem(own, other))


def collect_kernel(seqs, experts, kept, *refs):
    result = refs[-1]
    total = kept[...]
    for ref in refs[:-1]:
        total += ref[...].astype(F32)
    total = total.astype(BF16)
    per_expert = total.shape[0] // (seqs * experts)
    order = expert_order(seqs, experts, per_expert, True)
    result[...] = jnp.dot(order, total, preferred_element_type=F32).astype(BF16)


def collect(kept, parts, seqs, experts):
    return pl.pallas_call(
        functools.partial(collect_kernel, seqs, experts),
        in_specs=[WHOLE] * (1 + len(parts)),
        out_specs=WHOLE,
        out_shape=pltpu.VMEM(kept.shape, BF16),
        compiler_params=small(4),
        name="collect",
    )(*in_vmem(kept, *parts))


def stack_kernel(place, *refs):
    result = refs[-1]
    side = result.shape[0]
    for k, ref in enumerate(refs[:-1]):
        result[lax.rem(place[2] + side - k, side)] = ref[...]


def stack(place, pieces):
    return pl.pallas_call(
        stack_kernel,
        in_specs=[SCALARS] + [WHOLE] * len(pieces),
        out_specs=WHOLE,
        out_shape=pltpu.VMEM((len(pieces), *pieces[0].shape), BF16),
        compiler_params=small(4),
        name="stack",
    )(place, *in_vmem(*pieces))


def combine_kernel(source, seq, place, mix, *refs):
    lines, (result, slots, buffer, sems) = refs[:-4], refs[-4:]
    side, rows, _ = lines[0].shape
    seqs = slots.shape[0]
    owned = rows // seqs
    for k, line in enumerate(lines):
        column = lax.rem(place[3] + side - k, side) * owned
        for f in range(side):
            start = pl.multiple_of(f * side * owned + column, owned)
            for q in range(seqs):
                slots[q, pl.ds(start, owned), :] = line[f, q * owned : (q + 1) * owned, :]
    copies = []
    for b in range(result.shape[1]):
        chosen = slots[seq[b]]
        buffer[b] = jnp.dot(mix[source[b]], chosen, preferred_element_type=F32).astype(BF16)
        copies.append(pltpu.make_async_copy(buffer.at[b], result.at[0, b], sems.at[b]))
        copies[-1].start()
    for copy in copies:
        copy.wait()


def combine(source, seq, place, mixes, lines, seqs):
    _, block, slots = mixes.shape
    width = lines[0].shape[2]
    blocks = source.shape[0]
    return pl.pallas_call(
        combine_kernel,
        in_specs=[SCALARS, SCALARS, SCALARS] + [WHOLE] * (1 + len(lines)),
        out_specs=ANYWHERE,
        out_shape=pltpu.HBM((1, blocks, block, width), BF16),
        scratch_shapes=[
            pltpu.VMEM((seqs, slots, width), BF16),
            pltpu.VMEM((blocks, block, width), BF16),
            pltpu.SemaphoreType.DMA((blocks,)),
        ],
        compiler_params=small(16),
        name="combine",
    )(source, seq, place, *in_vmem(mixes, *lines))


def swapped(array):
    return lax.ppermute(array, "c", [(0, 1), (1, 0)])


def exchanged(array, axis):
    return lax.all_to_all(array, axis, split_axis=0, concat_axis=0, tiled=True)


def moved(array, axis, step):
    size = lax.axis_size(axis)
    return lax.ppermute(array, axis, [(i, (i + step) % size) for i in range(size)])


def along(array, first, step):
    side = lax.axis_size("z")
    pairs = []
    for c in range(lax.axis_size("c")):
        for z in range(side):
            for x in range(side):
                in_z = first == (c == 0)
                to_z, to_x = ((z + step) % side, x) if in_z else (z, (x + step) % side)
                pairs.append(((c * side + z) * side + x, (c * side + to_z) * side + to_x))
    return lax.ppermute(array, ("c",) + EXPERT, pairs)


def local(tokens, slot_params, dest, lengths, w_in, w_out):
    seqs, _ = tokens.shape[1:3]
    held = dest.shape[1] * dest.shape[2]
    side = lax.axis_size("z")
    experts = w_in.shape[0]
    owned = slot_params.shape[1] // (side * side)
    planes = lax.axis_size("y")
    z, x, core = lax.axis_index("z"), lax.axis_index("x"), lax.axis_index("c")
    swap = core == 1
    place = jnp.stack([z * side + x, core, jnp.where(swap, x, z), jnp.where(swap, z, x)])
    table = dest[0].T

    steps = range(1, side)
    parts = dispatch(tokens, slot_params, lengths, table, place, side)
    mixes = mix_rows(tokens, slot_params, lengths, table, place, side)
    parts = [parts[0]] + [along(parts[k], True, k) for k in steps]
    received = []
    for k in (*steps, 0):
        piece = merge(place, parts, k)
        received.append(along(piece, False, k) if k else piece)
    received = received[-1:] + received[:-1]
    arrived = exchanged(mixes, EXPERT)
    slot_in, tags = own_slots(received, seqs, experts, owned)
    weights = fetch(w_in, w_out)
    own = [slot_in] + [moved(slot_in, "y", k) for k in range(1, planes)]

    other = [swapped(piece) for piece in own]
    own_out, other_out = expert_layers(own, other, *weights)
    kept, *sent = join(own_out, swapped(other_out))
    parts = [moved(piece, "y", -k - 1) for k, piece in enumerate(sent)]
    slot_out = collect(kept, parts, seqs, experts)

    found = tags[:, TAGS : TAGS + side].astype(jnp.int32) - 1
    line = jnp.arange(side, dtype=jnp.int32)[None, :]
    across = (place[3] - jnp.arange(side, dtype=jnp.int32)[:, None]) % side
    shard = jnp.where(swap, across * side + line, line * side + across).reshape(-1)
    found = found.reshape(-1)
    block = jnp.where(found >= 0, found // seqs, -1)
    match = block[None, :] == jnp.arange(held, dtype=jnp.int32)[:, None]
    source = jnp.sum(jnp.where(match, shard[None, :], 0), axis=1)
    seq = jnp.sum(jnp.where(match, found[None, :] % seqs, 0), axis=1)

    pieces = stack(place, [slot_out] + [along(slot_out, True, k) for k in steps])
    lines = [pieces] + [along(pieces, False, k) for k in steps]
    return combine(source, seq, place, arrived, lines, seqs)


def solution(mesh):
    finer = Mesh(mesh.devices.reshape(4, 2, 4, 4), DP + EXPERT)
    in_specs = (
        P(DP, None, EXPERT, None),
        P(),
        P(DP, None, EXPERT),
        P(DP, None),
        P(EXPERT, None, DP),
        P(EXPERT, DP, None),
    )
    out_specs = P(DP, EXPERT, None, None)
    return jax.shard_map(local, mesh=finer, in_specs=in_specs, out_specs=out_specs, check_vma=False)
```
